256 devices in a mesh: ep: 32 (over z, y), dp: 8 (over x, core).
Axes of the slice: x: 4, y: 4, z: 8, core: 2. Of those that a mesh axis runs over, the one named last changes fastest.
Arguments:
- tokens: bfloat16 [8192, 512], P(('dp', 'ep'))
- d_out: bfloat16 [8192, 512], P(('dp', 'ep'))
- expert_ids: int32 [2, 8192, 6], P(None, ('dp', 'ep'))
- gate_vals: float32 [2, 8192, 6], P(None, ('dp', 'ep'))
- w_mix: bfloat16 [2, 512, 512], replicated
- w_gate: bfloat16 [2, 64, 512, 352], P(None, 'ep')
- w_up: bfloat16 [2, 64, 512, 352], P(None, 'ep')
- w_down: bfloat16 [2, 64, 352, 512], P(None, 'ep')
Outputs:
- output 1: bfloat16 [8192, 512], P(('dp', 'ep'))
- output 2: bfloat16 [8192, 512], P(('dp', 'ep'))
- output 3: bfloat16 [2, 512, 512], replicated
- output 4: bfloat16 [2, 64, 512, 352], P(None, 'ep')
- output 5: bfloat16 [2, 64, 512, 352], P(None, 'ep')
- output 6: bfloat16 [2, 64, 352, 512], P(None, 'ep')
All inputs are finite; a program needn't handle non-finite values.
Results may differ from the reference program's by a relative error of at most 0.02.
Values are sent between devices in bfloat16 or wider.
A program may use at most 768 MiB of HBM per device.

```python
import jax
import jax.numpy as jnp

D = 512
FF = 352
EXPERTS = 64
TOP = 6
TOK = 32
NDEV = 256
LAYERS = 2
CAP = 9
HOT = 8

N_TOK = TOK * NDEV
CAP_ALL = CAP * NDEV


def route_device(hot_mask, dev_key):
    key_rest, key_run, key_tok = jax.random.split(dev_key, 3)
    rest_copies = TOK * TOP - HOT * CAP
    base_count = rest_copies // (EXPERTS - HOT)
    extra_count = rest_copies % (EXPERTS - HOT)
    shuffled = jax.random.permutation(key_rest, EXPERTS)
    cold_sorted = 1 - hot_mask[shuffled]
    cold_rank = jnp.cumsum(cold_sorted) - 1
    bonus_sorted = cold_sorted * (cold_rank < extra_count).astype(jnp.int32)
    bonus = jnp.zeros((EXPERTS,), jnp.int32).at[shuffled].set(bonus_sorted)
    counts = jnp.where(hot_mask == 1, CAP, base_count + bonus)
    run_order = jax.random.permutation(key_run, EXPERTS)
    flat_ids = jnp.repeat(run_order, counts[run_order], total_repeat_length=TOK * TOP)
    table = flat_ids.reshape(TOP, TOK).T
    return table[jax.random.permutation(key_tok, TOK)]


def route_layer(layer_key):
    key_hot, key_dev = jax.random.split(layer_key)
    hot_ids = jax.random.permutation(key_hot, EXPERTS)[:HOT]
    hot_mask = jnp.zeros((EXPERTS,), jnp.int32).at[hot_ids].set(1)
    per_device = jax.vmap(route_device, in_axes=(None, 0))(hot_mask, jax.random.split(key_dev, NDEV))
    return per_device.reshape(N_TOK, TOP)


def setup_inputs(seed: int = 0) -> dict:
    keys = jax.random.split(jax.random.key(seed), 8)
    tokens = jax.random.normal(keys[0], (N_TOK, D), jnp.float32).astype(jnp.bfloat16)
    d_out = jax.random.normal(keys[1], (N_TOK, D), jnp.float32).astype(jnp.bfloat16)
    expert_ids = jax.vmap(route_layer)(jax.random.split(keys[2], LAYERS))
    gate_vals = jax.random.uniform(keys[3], (LAYERS, N_TOK, TOP), jnp.float32, 0.5, 1.5) * TOP ** -0.5
    w_mix = (jax.random.normal(keys[4], (LAYERS, D, D), jnp.float32) * D ** -0.5).astype(jnp.bfloat16)
    w_gate = (jax.random.normal(keys[5], (LAYERS, EXPERTS, D, FF), jnp.float32) * D ** -0.5).astype(jnp.bfloat16)
    w_up = (jax.random.normal(keys[6], (LAYERS, EXPERTS, D, FF), jnp.float32) * D ** -0.5).astype(jnp.bfloat16)
    w_down = (jax.random.normal(keys[7], (LAYERS, EXPERTS, FF, D), jnp.float32) * FF ** -0.5).astype(jnp.bfloat16)
    return {'tokens': tokens, 'd_out': d_out, 'expert_ids': expert_ids, 'gate_vals': gate_vals,
            'w_mix': w_mix, 'w_gate': w_gate, 'w_up': w_up, 'w_down': w_down}


def silu_parts(pre_gate):
    sig_val = jax.nn.sigmoid(pre_gate)
    return pre_gate * sig_val, sig_val * (1.0 + pre_gate * (1.0 - sig_val))


def copy_slots(expert_ids):
    flat_ids = expert_ids.reshape(-1)
    sort_order = jnp.argsort(flat_ids, stable=True)
    sorted_ids = flat_ids[sort_order]
    counts = jnp.bincount(flat_ids, length=EXPERTS)
    starts = jnp.cumsum(counts) - counts
    rows_sorted = sorted_ids * CAP_ALL + jnp.arange(flat_ids.shape[0]) - starts[sorted_ids]
    return jnp.zeros_like(flat_ids).at[sort_order].set(rows_sorted)


def layer_forward(x_in, expert_ids, gate_vals, w_mix, w_gate, w_up, w_down):
    mixed = x_in.astype(jnp.float32) + jnp.dot(x_in, w_mix, preferred_element_type=jnp.float32)
    u_act = mixed.astype(jnp.bfloat16)
    copy_rows = copy_slots(expert_ids)
    copy_tok = jnp.arange(N_TOK * TOP) // TOP
    expert_in = jnp.zeros((EXPERTS * CAP_ALL, D), jnp.bfloat16).at[copy_rows].set(u_act[copy_tok])
    expert_in = expert_in.reshape(EXPERTS, CAP_ALL, D)
    expert_f = expert_in.astype(jnp.float32)
    pre_gate = jnp.einsum('ecd,edf->ecf', expert_f, w_gate.astype(jnp.float32))
    pre_up = jnp.einsum('ecd,edf->ecf', expert_f, w_up.astype(jnp.float32))
    act, _ = silu_parts(pre_gate)
    hidden = (act * pre_up).astype(jnp.bfloat16)
    expert_out = jnp.einsum('ecf,efd->ecd', hidden.astype(jnp.float32), w_down.astype(jnp.float32)).astype(jnp.bfloat16)
    out_copy = expert_out.reshape(EXPERTS * CAP_ALL, D)[copy_rows].reshape(N_TOK, TOP, D)
    y_out = u_act.astype(jnp.float32) + jnp.sum(gate_vals[:, :, None] * out_copy.astype(jnp.float32), axis=1)
    return y_out.astype(jnp.bfloat16), (x_in, copy_rows, expert_in, pre_gate, pre_up, hidden)


def layer_backward(saved, d_y, gate_vals, w_mix, w_gate, w_up, w_down):
    x_in, copy_rows, expert_in, pre_gate, pre_up, hidden = saved
    g_dy = (gate_vals[:, :, None] * d_y.astype(jnp.float32)[:, None, :]).astype(jnp.bfloat16).reshape(N_TOK * TOP, D)
    d_buf = jnp.zeros((EXPERTS * CAP_ALL, D), jnp.bfloat16).at[copy_rows].set(g_dy).reshape(EXPERTS, CAP_ALL, D)
    d_buf_f = d_buf.astype(jnp.float32)
    d_hidden = jnp.einsum('ecd,efd->ecf', d_buf_f, w_down.astype(jnp.float32))
    act, act_slope = silu_parts(pre_gate)
    d_pre_gate = (d_hidden * pre_up * act_slope).astype(jnp.bfloat16).astype(jnp.float32)
    d_pre_up = (d_hidden * act).astype(jnp.bfloat16).astype(jnp.float32)
    d_expert_in = (jnp.einsum('ecf,edf->ecd', d_pre_gate, w_gate.astype(jnp.float32))
                   + jnp.einsum('ecf,edf->ecd', d_pre_up, w_up.astype(jnp.float32))).astype(jnp.bfloat16)
    expert_f = expert_in.astype(jnp.float32)
    g_gate = jnp.einsum('ecd,ecf->edf', expert_f, d_pre_gate).astype(jnp.bfloat16)
    g_up = jnp.einsum('ecd,ecf->edf', expert_f, d_pre_up).astype(jnp.bfloat16)
    g_down = jnp.einsum('ecf,ecd->efd', hidden.astype(jnp.float32), d_buf_f).astype(jnp.bfloat16)
    d_copy = d_expert_in.reshape(EXPERTS * CAP_ALL, D)[copy_rows].reshape(N_TOK, TOP, D)
    d_u = (d_y.astype(jnp.float32) + jnp.sum(gate_vals[:, :, None] * d_copy.astype(jnp.float32), axis=1)).astype(jnp.bfloat16)
    g_mix = jnp.dot(x_in.T, d_u, preferred_element_type=jnp.float32).astype(jnp.bfloat16)
    d_x = (d_u.astype(jnp.float32) + jnp.dot(d_u, w_mix.T, preferred_element_type=jnp.float32)).astype(jnp.bfloat16)
    return d_x, (g_mix, g_gate, g_up, g_down)


def reference(tokens, d_out, expert_ids, gate_vals, w_mix, w_gate, w_up, w_down):
    layer_in = tokens
    saved_all = []
    for layer in range(LAYERS):
        layer_in, saved = layer_forward(layer_in, expert_ids[layer], gate_vals[layer], w_mix[layer],
                                        w_gate[layer], w_up[layer], w_down[layer])
        saved_all.append(saved)
    d_y = d_out
    grads = []
    for layer in reversed(range(LAYERS)):
        d_y, grad_set = layer_backward(saved_all[layer], d_y, gate_vals[layer], w_mix[layer],
                                       w_gate[layer], w_up[layer], w_down[layer])
        grads.insert(0, grad_set)
    return (layer_in, d_y,
            jnp.stack([entry[0] for entry in grads]),
            jnp.stack([entry[1] for entry in grads]),
            jnp.stack([entry[2] for entry in grads]),
            jnp.stack([entry[3] for entry in grads]))
```

```python
import functools

import jax
import jax.numpy as jnp
from jax import lax
from jax.experimental import pallas as pl
from jax.experimental.pallas import tpu as pltpu
from jax.sharding import PartitionSpec as P

NZ, NY, NX = 8, 4, 4
T = 32
D = 512
FF, FP = 352, 384
GR = 3 * FF
HR = GR // 2
NT = NZ * NY * T
CH = NY * T
SL = D // (NZ * NY)
BF, F32 = jnp.bfloat16, jnp.float32
MESH = pl.DeviceIdType.MESH
PLUS, MINUS = 0, 1
SIGN = (1, -1)
LANES = 128
ZSEM = (2, 4, 4)


def vmem(dims, dtype=BF):
    return pltpu.VMEM(dims, dtype)


def both(*dims):
    return (2, 2, *dims)


def dot(a, b, ca=1, cb=0):
    return lax.dot_general(a, b, (((ca,), (cb,)), ((), ())), preferred_element_type=F32)


def dot_nt(a, b):
    return dot(a, b, 1, 1)


def dot_tn(a, b):
    return dot(a, b, 0, 0)


def lim(direction, unit):
    return 4 if (unit < 2) == (direction == PLUS) else 3


def step_kernel(tok, dout, ids, gates, wmix, wg_hbm, wu_hbm, wd_hbm,
                y_out, dx_out, dmix_out, dg_out, du_out, dw_out,
                w3, x1, x2, dyg, du2, du1, u1, u2, gt, ab, hb, dab, cb_, pacc, pacc2,
                rs_first, rs_recv, rs_fin, rs_ys, rs_yr,
                grad, rd, rg, fin,
                dm_full, dm_send, dm_recv, dm_all,
                w_sem, ag_ys, ag_yr, ag_zs, ag_zr, rs_s, rs_r, rs_ysm, rs_yrm,
                ar_s, ar_r, dx_s, dx_r, out_sem, dy_s, dy_r):
    ep = lax.axis_index('ep')
    dp = lax.axis_index('dp')
    z, y = lax.div(ep, NY), lax.rem(ep, NY)
    x, core = lax.div(dp, 2), lax.rem(dp, 2)

    z_at = [lax.rem(z + i, NZ) for i in range(NZ)]
    y_at = [lax.rem(y + i, NY) for i in range(NY)]
    x_at = [lax.rem(x + i, NX) for i in range(NX)]
    ep_at = [[zz * NY + yy for yy in y_at] for zz in z_at]
    rows_at = {rows: [[pl.multiple_of(v * rows, rows) for v in line] for line in ep_at] for rows in (T, SL)}
    plane_at = [zz * NY for zz in z_at]
    home_at = [[pl.multiple_of((zz + yd) * T, T) for yd in range(NY)] for zz in plane_at]
    unit_at = [pl.multiple_of(yy * T, T) for yy in y_at]
    dp_x = [xx * 2 + core for xx in x_at]
    dp_r = [lax.rem(dp + r, 8) for r in range(8)]
    partner = dp + 1 - 2 * core
    q128 = [pl.multiple_of(xx * 128, 128) for xx in x_at]
    q64 = [[pl.multiple_of(xx * 128 + 64 * h, 64) for h in range(2)] for xx in x_at]

    def ep_of(dz, dy):
        return ep_at[dz % NZ][dy % NY]

    def dp_of(dx):
        return dp_x[dx % NX]

    def remote(src, dst, ssem, rsem, ep_to=None, dp_to=None):
        return pltpu.make_async_remote_copy(
            src_ref=src, dst_ref=dst, send_sem=ssem, recv_sem=rsem,
            device_id=(ep if ep_to is None else ep_to, dp if dp_to is None else dp_to),
            device_id_type=MESH)

    barrier = pltpu.get_barrier_semaphore()
    peers = [(ep_of(0, j), dp) for j in range(1, NY)]
    peers += [(ep_of(1, 0), dp), (ep_of(-1, 0), dp)]
    peers += [(ep, dp_r[r]) for r in range(1, 8)]
    for peer in peers:
        pl.semaphore_signal(barrier, inc=1, device_id=peer, device_id_type=MESH)

    loads = []
    for p, src in enumerate((wg_hbm, wu_hbm, wd_hbm)):
        for l in range(2):
            for e in range(2):
                loads.append(pltpu.make_async_copy(src.at[l, e], w3.at[l, e, pl.ds(FP * p, FF), :],
                                                   w_sem.at[p, l, e]))
    for load in loads:
        load.start()

    class Gather:
        def __init__(self, view, s, r):
            self.view, self.s, self.r = view, s, r

        def block(self, dz, dy):
            return self.view(dz % NZ, dy % NY)

        def ycopy(self, j, from_j):
            blk = self.block(0, -from_j)
            return remote(blk, blk, ag_ys.at[self.s, j - 1], ag_yr.at[self.r, j - 1], ep_to=ep_of(0, j))

        def zcopy(self, direction, dist, j, arriving):
            sign = SIGN[direction]
            blk = self.block(-sign * (dist if arriving else dist - 1), -j)
            return remote(blk, blk, ag_zs.at[self.s, direction, dist - 1, j],
                          ag_zr.at[self.r, direction, dist - 1, j], ep_to=ep_of(sign, 0))

        def start(self):
            for direction in (PLUS, MINUS):
                self.zcopy(direction, 1, 0, False).start()
            for j in range(1, NY):
                self.ycopy(j, 0).start()

        def y_arrive(self):
            for j in (1, 3, 2):
                self.ycopy(j, j).wait_recv()
                for direction in (PLUS, MINUS):
                    self.zcopy(direction, 1, j, False).start()

        def poll(self, p):
            dist = p // 2 + 1
            for j in (2 * (p % 2), 2 * (p % 2) + 1):
                for direction in (PLUS, MINUS):
                    if dist <= lim(direction, j):
                        self.zcopy(direction, dist, j, True).wait_recv()
                        if dist < lim(direction, j):
                            self.zcopy(direction, dist + 1, j, False).start()

        def chunk(self, k):
            if k == 0:
                self.y_arrive()
            elif k == 1:
                self.poll(0)
            if k > 0:
                self.poll(k)

        def drain(self):
            for j in range(1, NY):
                self.ycopy(j, 0).wait_send()
            for direction in (PLUS, MINUS):
                for j in range(NY):
                    for dist in range(1, lim(direction, j) + 1):
                        self.zcopy(direction, dist, j, False).wait_send()

    class ColumnGather:
        def zcopy(self, direction, dist, arriving):
            sign = SIGN[direction]
            zz = z_at[(-sign * (dist if arriving else dist - 1)) % NZ]
            blk = dyg.at[zz, pl.ds(unit_at[0], T), :]
            return remote(blk, blk, dy_s.at[direction, dist - 1], dy_r.at[direction, dist - 1], ep_to=ep_of(sign, 0))

        def ycopy(self, direction, hop, arriving):
            sign = SIGN[direction]
            col = unit_at[(-sign * (hop if arriving else hop - 1)) % NY]
            planes = pl.ds(0, NZ) if hop == 1 else pl.ds(4 * direction, 4)
            blk = dyg.at[planes, pl.ds(col, T), :]
            return remote(blk, blk, dy_s.at[direction, 3 + hop], dy_r.at[direction, 3 + hop], ep_to=ep_of(0, sign))

        def start(self):
            for direction in (PLUS, MINUS):
                self.zcopy(direction, 1, False).start()

        def zpoll(self, dist):
            for direction in (PLUS, MINUS):
                if dist <= 4 - direction:
                    self.zcopy(direction, dist, True).wait_recv()
                    if dist < 4 - direction:
                        self.zcopy(direction, dist + 1, False).start()
            if dist == 4:
                for direction in (PLUS, MINUS):
                    self.ycopy(direction, 1, False).start()

        def ypoll(self, hop):
            for direction in (PLUS, MINUS):
                self.ycopy(direction, hop, True).wait_recv()
                if hop == 1:
                    self.ycopy(direction, 2, False).start()

        def drain(self):
            for direction in (PLUS, MINUS):
                for dist in range(1, 5 - direction):
                    self.zcopy(direction, dist, False).wait_send()
                for hop in (1, 2):
                    self.ycopy(direction, hop, False).wait_send()

    class Scatter:
        def __init__(self, part, n):
            self.part, self.n = part, n

        def rows(self, dz, yd):
            return pl.ds(home_at[dz % NZ][yd], T)

        def zcopy(self, direction, s, yd):
            sign = SIGN[direction]
            unit = pl.ds(yd * T, T)
            n = self.n
            src = rs_first.at[n, direction, unit, :] if s == 0 else rs_recv.at[n, direction, s - 1, unit, :]
            last = s == lim(direction, yd) - 1
            dst = rs_fin.at[n, direction, unit, :] if last else rs_recv.at[n, direction, s, unit, :]
            return remote(src, dst, rs_s.at[n // 3, direction, s, yd], rs_r.at[n, direction, s, yd], ep_to=ep_of(sign, 0))

        def round(self, s):
            for yd in range(NY):
                for direction in (PLUS, MINUS):
                    hops = lim(direction, yd)
                    sign = SIGN[direction]
                    if s > hops:
                        continue
                    if s > 0:
                        self.zcopy(direction, s - 1, yd).wait_recv()
                    if s == hops:
                        continue
                    unit = pl.ds(yd * T, T)
                    mine = self.part[self.rows(sign * (hops - s), yd), :]
                    if s == 0:
                        rs_first[self.n, direction, unit, :] = mine.astype(BF)
                    else:
                        got = rs_recv[self.n, direction, s - 1, unit, :]
                        rs_recv[self.n, direction, s - 1, unit, :] = (mine + got.astype(F32)).astype(BF)
                    self.zcopy(direction, s, yd).start()

        def plane(self, dy):
            unit = pl.ds(unit_at[dy % NY], T)
            return (self.part[pl.ds(rows_at[T][0][dy % NY], T), :] + rs_fin[self.n, PLUS, unit, :].astype(F32)
                    + rs_fin[self.n, MINUS, unit, :].astype(F32))

        def ycopy(self, j):
            return remote(rs_ys.at[self.n, j - 1], rs_yr.at[self.n, j - 1], rs_ysm.at[self.n // 3, j - 1],
                          rs_yrm.at[self.n, j - 1], ep_to=ep_of(0, j))

        def y_start(self):
            for j in range(1, NY):
                rs_ys[self.n, j - 1] = self.plane(j).astype(BF)
                self.ycopy(j).start()

        def finish(self):
            total = self.plane(0)
            for j in range(1, NY):
                self.ycopy(j).wait_recv()
                total = total + rs_yr[self.n, j - 1].astype(F32)
            for yd in range(NY):
                for direction in (PLUS, MINUS):
                    for s in range(lim(direction, yd)):
                        self.zcopy(direction, s, yd).wait_send()
            for j in range(1, NY):
                self.ycopy(j).wait_send()
            return total

    class Reduce:
        def __init__(self, n):
            self.n = n

        def copy(self, src, dst, slot, dp_to):
            return remote(src, dst, ar_s.at[self.n, slot], ar_r.at[self.n, slot], dp_to=dp_to)

        def swap(self):
            n = self.n
            return self.copy(grad.at[n, 1 - core, pl.ds(0, GR), :], rd.at[n], 0, partner)

        def part(self, q, h):
            return rd.at[self.n, pl.ds(HR * h, HR), pl.ds(q128[q % NX], LANES)]

        def slot(self, i):
            return rg.at[self.n, i]

        def scatter_copy(self, i):
            right, left = dp_of(1), dp_of(-1)
            src = self.slot(i - 4) if i >= 4 else self.part(*((2, 0), (-2, 1), (-1, 0), (1, 1))[i])
            to = [right, left, left, right, right, left][i]
            return self.copy(src, self.slot(i), 1 + i, to)

        def fin(self, q, h=None):
            rows = pl.ds(0, GR) if h is None else pl.ds(HR * h, HR)
            return fin.at[self.n, core, rows, pl.ds(q128[q % NX], LANES)]

        def gather_copy(self, i, arriving=False):
            right, left = dp_of(1), dp_of(-1)
            sent = [(0, None), (0, None), (-1, 0), (1, 1)][i]
            came = [(-1, None), (1, None), (-2, 0), (2, 1)][i]
            ref = self.fin(*(came if arriving else sent))
            return self.copy(ref, ref, 7 + i, [right, left, right, left][i])

        def back(self, arriving=False):
            ref = fin.at[self.n, 1 - core if arriving else core]
            return self.copy(ref, ref, 11, partner)

        def out(self):
            return [pltpu.make_async_copy(fin.at[self.n, e, pl.ds(FF * p, FF), :], dst.at[self.n, e],
                                          out_sem.at[self.n, e, p])
                    for e in range(2) for p, dst in enumerate((dg_out, du_out, dw_out))]

        def stage(self, i):
            n = self.n
            if i == 0:
                self.swap().start()
            elif i == 1:
                self.swap().wait_recv()

                @pl.loop(0, 3)
                def _(r):
                    rows = pl.ds(pl.multiple_of(r * FF, FF), FF)
                    rd[n, rows, :] = (rd[n, rows, :].astype(F32) + grad[n, core, rows, :].astype(F32)).astype(BF)

                for i2 in range(4):
                    self.scatter_copy(i2).start()
            elif i == 2:
                for i2, q, h in ((0, 1, 0), (1, -1, 1)):
                    self.scatter_copy(i2).wait_recv()
                    got = self.slot(i2)
                    got[...] = (got[...].astype(F32) + self.part(q, h)[...].astype(F32)).astype(BF)
                    self.scatter_copy(4 + i2).start()
            elif i == 3:
                for i2 in (2, 3, 4, 5):
                    self.scatter_copy(i2).wait_recv()
                for h in range(2):
                    self.fin(0, h)[...] = (self.part(0, h)[...].astype(F32) + self.slot(2 + h)[...].astype(F32)
                                           + self.slot(4 + h)[...].astype(F32)).astype(BF)
                self.gather_copy(0).start()
                self.gather_copy(1).start()
            elif i == 4:
                for i2 in range(2):
                    self.gather_copy(i2, True).wait_recv()
                    self.gather_copy(2 + i2).start()
            elif i == 5:
                self.gather_copy(2, True).wait_recv()
                self.gather_copy(3, True).wait_recv()
                self.back().start()
            elif i == 6:
                self.back(True).wait_recv()
                for c in self.out():
                    c.start()
                for i2 in range(6):
                    self.scatter_copy(i2).wait_send()
                for i2 in range(4):
                    self.gather_copy(i2).wait_send()
                self.swap().wait_send()
                self.back().wait_send()
            elif i == 7:
                for c in self.out():
                    c.wait()

    slice_rows = pl.ds(pl.multiple_of(lax.rem(ep, 8) * SL, SL), SL)

    def mix_copy(n, r):
        return remote(dm_send.at[n], dm_recv.at[n, r - 1], dx_s.at[n, r - 1], dx_r.at[n, r - 1], dp_to=dp_r[r])

    def mix_start(n, xg, dug):
        lanes = pl.ds(pl.multiple_of(lax.div(ep, 8) * 128, 128), 128)
        dm_full[n] = dot_tn(xg[:, lanes], dug[...])
        dm_send[n] = dm_full[n, slice_rows, :].astype(BF)
        for r in range(1, 8):
            mix_copy(n, r).start()

    def mix_sum(n):
        own = pl.ds(rows_at[SL][0][0], SL)
        total = dm_full[n, slice_rows, :]
        for r in range(1, 8):
            mix_copy(n, r).wait_recv()
            total = total + dm_recv[n, r - 1].astype(F32)
        dm_all[n, own, :] = total.astype(BF)
        for r in range(1, 8):
            mix_copy(n, r).wait_send()

    own_rows = pl.ds(rows_at[T][0][0], T)
    home_unit = pl.ds(unit_at[0], T)

    def plane_rows(k):
        return pl.ds(pl.multiple_of(plane_of(k) * CH, CH), CH)

    def plane_of(k):
        odd = lax.rem(k, 2)
        dist = lax.div(k + 1, 2)
        return lax.rem(z + NZ - odd * dist + (1 - odd) * dist, NZ)

    def gate_col(layer, e, rows):
        table = gt[rows, :]
        lane = lax.broadcasted_iota(jnp.int32, (CH, 128), 1)
        return jnp.sum(jnp.where(lane == layer * 64 + ep * 2 + e, table, 0.0), axis=1, keepdims=True)

    def expert_in(u, gcol):
        return jnp.where(gcol > 0.0, u, 0.0).astype(BF)

    x1[own_rows, :] = tok[...]
    slot = lax.broadcasted_iota(jnp.int32, (LANES, T), 0)
    table = jnp.zeros((LANES, T), F32)
    for l in range(2):
        for j in range(6):
            table = table + jnp.where(slot == ids[j, l:l + 1, :] + 64 * l, gates[j, l:l + 1, :], 0.0)
    gt[own_rows, :] = table.T
    dyg[z, home_unit, :] = dout[...]
    pl.semaphore_wait(barrier, len(peers))

    def row_view(buf):
        return lambda dz, dy: buf.at[pl.ds(rows_at[T][dz][dy], T), :]

    ag_tok = Gather(row_view(x1), 0, 0)
    ag_gt = Gather(row_view(gt), 1, 1)
    ag_dy = ColumnGather()
    ag_x2 = Gather(row_view(x2), 0, 2)
    ag_du2 = Gather(row_view(du2), 1, 3)
    ag_du1 = Gather(row_view(du1), 0, 4)
    ag_mix = Gather(lambda dz, dy: dm_all.at[:, pl.ds(rows_at[SL][dz][dy], SL), :], 1, 5)
    ag_tok.start()
    ag_gt.start()
    ag_dy.start()

    for load in loads:
        load.wait()
    for l in range(2):
        for e in range(2):
            for p in range(3):
                w3[l, e, FP * p + FF:FP * p + FP, :] = jnp.zeros((FP - FF, D), BF)

    def gate_up(l, e):
        return w3[l, e, 0:2 * FP, :]

    def down(l, e):
        return w3[l, e, 2 * FP:, :]

    @pl.loop(0, 8)
    def _(k):
        for kk in range(8):
            @pl.when(k == kk)
            def _(kk=kk):
                ag_tok.chunk(kk)
                ag_gt.chunk(kk)
                if kk in (1, 3, 5, 7):
                    ag_dy.zpoll((kk + 1) // 2)
        rows = plane_rows(k)
        xc = x1[rows, :]
        u = (xc.astype(F32) + dot(xc, wmix[0])).astype(BF)
        u1[rows, :] = u
        uf = u.astype(F32)
        total = jnp.zeros((CH, D), F32)
        for e in range(2):
            gcol = gate_col(0, e, rows)
            pre = dot_nt(expert_in(uf, gcol), gate_up(0, e))
            ab[e, rows, :] = pre
            a, b = pre[:, :FP], pre[:, FP:]
            h = (a * jax.nn.sigmoid(a) * b).astype(BF)
            hb[0, e, rows, :] = h
            total = total + gcol * dot(h, down(0, e)).astype(BF).astype(F32)
        pacc[rows, :] = total

    rs = Scatter(pacc, 0)
    for s in range(5):
        rs.round(s)
        if s in (2, 4):
            ag_dy.ypoll(s // 2)
    rs.y_start()
    ag_tok.drain()
    ag_gt.drain()
    ag_dy.drain()
    y1 = (u1[own_rows, :].astype(F32) + rs.finish()).astype(BF)
    x2[own_rows, :] = y1
    ag_x2.start()

    def backward_part(layer, e, rows, gcol, dyc, pre):
        a, b = pre[:, :FP], pre[:, FP:]
        c = (gcol * dyc).astype(BF)
        cb_[e, rows, :] = c
        dh = dot_nt(c, down(layer, e))
        s = jax.nn.sigmoid(a)
        dab[e, rows, 0:FP] = (dh * b * (s * (1.0 + a * (1.0 - s)))).astype(BF)
        dab[e, rows, FP:] = (dh * (a * s)).astype(BF)
        v = dot(dab[e, rows, :], gate_up(layer, e)).astype(BF)
        return gcol * v.astype(F32)

    @pl.loop(0, 8)
    def _(k):
        for kk in range(8):
            @pl.when(k == kk)
            def _(kk=kk):
                ag_x2.chunk(kk)
        rows = plane_rows(k)
        xc = x2[rows, :]
        u = (xc.astype(F32) + dot(xc, wmix[1])).astype(BF)
        u2[rows, :] = u
        uf = u.astype(F32)
        dyc = dyg[plane_of(k)].astype(F32)
        total = jnp.zeros((CH, D), F32)
        back = jnp.zeros((CH, D), F32)
        for e in range(2):
            gcol = gate_col(1, e, rows)
            pre = dot_nt(expert_in(uf, gcol), gate_up(1, e))
            a, b = pre[:, :FP], pre[:, FP:]
            h = (a * jax.nn.sigmoid(a) * b).astype(BF)
            hb[1, e, rows, :] = h
            total = total + gcol * dot(h, down(1, e)).astype(BF).astype(F32)
            back = back + backward_part(1, e, rows, gcol, dyc, pre)
        pacc2[rows, :] = total
        pacc[rows, :] = back

    def weight_grads(layer, e, ug):
        @pl.loop(0, 6)
        def _(i):
            part = lax.div(i, 3)
            cols = pl.ds(pl.multiple_of(i * LANES, LANES), LANES)
            rows = pl.ds(pl.multiple_of(part * FF + (i - 3 * part) * LANES, 32), LANES)
            grad[layer, e, rows, :] = dot_tn(dab[e, :, cols], ug[...]).astype(BF)

        @pl.loop(0, 3)
        def _(i):
            cols = pl.ds(pl.multiple_of(i * LANES, LANES), LANES)
            rows = pl.ds(pl.multiple_of(2 * FF + i * LANES, 32), LANES)
            grad[layer, e, rows, :] = dot_tn(hb[layer, e, :, cols], cb_[e]).astype(BF)

    rs = Scatter(pacc, 1)
    rs.round(0)
    weight_grads(1, 0, u2)
    rs.round(1)
    weight_grads(1, 1, u2)
    ar2 = Reduce(1)
    ar2.stage(0)
    for s in range(2, 5):
        rs.round(s)
    rs.y_start()
    ag_x2.drain()
    du2[own_rows, :] = (dout[...].astype(F32) + rs.finish()).astype(BF)
    ag_du2.start()
    ar2.stage(1)

    rs_y2 = Scatter(pacc2, 3)

    @pl.loop(0, 8)
    def _(k):
        for kk in range(8):
            @pl.when(k == kk)
            def _(kk=kk):
                ag_du2.chunk(kk)
                if kk in (2, 5):
                    rs_y2.round(kk // 3)
                if kk == 4:
                    ar2.stage(2)
        rows = plane_rows(k)
        duc = du2[rows, :]
        dyc = (duc.astype(F32) + dot_nt(duc, wmix[1])).astype(BF)
        dyg[plane_of(k)] = dyc
        dyc = dyc.astype(F32)
        back = jnp.zeros((CH, D), F32)
        for e in range(2):
            back = back + backward_part(0, e, rows, gate_col(0, e, rows), dyc, ab[e, rows, :])
        pacc[rows, :] = back

    rs = Scatter(pacc, 2)
    rs.round(0)
    ar2.stage(3)
    weight_grads(0, 0, u1)
    rs.round(1)
    weight_grads(0, 1, u1)
    ar1 = Reduce(0)
    ar1.stage(0)
    rs_y2.round(2)
    rs.round(2)
    mix_start(1, x2, du2)
    ar1.stage(1)
    rs.round(3)
    ar2.stage(4)
    rs_y2.round(3)
    rs.round(4)
    rs.y_start()
    ag_du2.drain()
    mix_sum(1)
    d_u1 = (dyg[z, home_unit, :].astype(F32) + rs.finish()).astype(BF)
    du1[own_rows, :] = d_u1
    ag_du1.start()
    dx_out[...] = (d_u1.astype(F32) + dot_nt(d_u1, wmix[0])).astype(BF)

    rs_y2.round(4)
    rs_y2.y_start()
    ag_du1.chunk(0)
    ar2.stage(5)
    for k in range(1, 4):
        ag_du1.chunk(k)
    ar1.stage(2)
    for k in range(4, 6):
        ag_du1.chunk(k)
    ar2.stage(6)
    for k in range(6, 8):
        ag_du1.chunk(k)
    mix_start(0, x1, du1)
    y_out[...] = (u2[own_rows, :].astype(F32) + rs_y2.finish()).astype(BF)
    ar1.stage(3)
    mix_sum(0)
    ag_mix.start()
    for k in range(3):
        ag_mix.chunk(k)
    ar1.stage(4)
    for k in range(3, 6):
        ag_mix.chunk(k)
    ar1.stage(5)
    for k in range(6, 8):
        ag_mix.chunk(k)
    dmix_out[...] = dm_all[...]
    ar1.stage(6)
    ar2.stage(7)
    ar1.stage(7)
    ag_du1.drain()
    ag_mix.drain()


def copy_kernel(*refs):
    n = len(refs) // 3
    src, dst, buf, sem = refs[:n], refs[n:2 * n], refs[2 * n:3 * n], refs[3 * n]
    loads = [pltpu.make_async_copy(src[i], buf[i], sem.at[0, i]) for i in range(n)]
    stores = [pltpu.make_async_copy(buf[i], dst[i], sem.at[1, i]) for i in range(n)]
    for load in loads:
        load.start()
    for load, store in zip(loads, stores):
        load.wait()
        store.start()
    for store in stores:
        store.wait()


def solution(mesh):
    tok_spec = P(('dp', 'ep'))
    route_spec = P(None, ('dp', 'ep'))
    whole_spec = P()
    expert_spec = P(None, 'ep')

    def device_step(tokens, d_out, expert_ids, gate_vals, w_mix, w_gate, w_up, w_down):
        vm = pl.BlockSpec(memory_space=pltpu.VMEM)
        hbm = pl.BlockSpec(memory_space=pl.ANY)
        shape = jax.ShapeDtypeStruct
        dma = pltpu.SemaphoreType.DMA
        wg_t, wu_t = jnp.swapaxes(w_gate, 2, 3), jnp.swapaxes(w_up, 2, 3)
        results = pl.pallas_call(
            step_kernel,
            out_shape=(shape((T, D), BF), shape((T, D), BF), shape((2, D, D), BF),
                       *[shape(both(FF, D), BF)] * 3),
            in_specs=[vm] * 5 + [hbm] * 3,
            out_specs=(vm,) * 3 + (hbm,) * 3,
            scratch_shapes=[
                vmem(both(3 * FP, D)),
                *[vmem((NT, D))] * 2, vmem((NZ, CH, D)), *[vmem((NT, D))] * 4,
                vmem((NT, LANES), F32), vmem((2, NT, 2 * FP), F32),
                vmem(both(NT, FP)), vmem((2, NT, 2 * FP)), vmem((2, NT, D)),
                vmem((NT, D), F32), vmem((NT, D), F32),
                vmem((4, 2, CH, D)), vmem((4, 2, 3, CH, D)), vmem((4, 2, CH, D)),
                vmem((4, 3, T, D)), vmem((4, 3, T, D)),
                vmem(both(GR + 32, D)), vmem((2, GR, D)), vmem((2, 6, HR, LANES)), vmem(both(GR, D)),
                vmem((2, LANES, D), F32), vmem((2, SL, D)), vmem((2, 7, SL, D)), vmem((2, D, D)),
                dma((3, 2, 2)),
                dma((2, 3)), dma((6, 3)), dma((2, *ZSEM)), dma((6, *ZSEM)),
                dma((2, *ZSEM)), dma((4, *ZSEM)), dma((2, 3)), dma((4, 3)),
                dma((2, 12)), dma((2, 12)), dma((2, 7)), dma((2, 7)), dma((2, 2, 3)), dma((2, 6)), dma((2, 6)),
            ],
            compiler_params=pltpu.CompilerParams(
                collective_id=0, has_side_effects=True, vmem_limit_bytes=67043328),
        )(tokens, d_out, jnp.transpose(expert_ids, (2, 0, 1)), jnp.transpose(gate_vals, (2, 0, 1)),
          w_mix, wg_t, wu_t, w_down)
        y, dx, dmix, dg_t, du_t, dw = pl.pallas_call(
            copy_kernel,
            out_shape=[shape(r.shape, r.dtype) for r in results],
            in_specs=[hbm] * 6,
            out_specs=[hbm] * 6,
            scratch_shapes=[vmem(r.shape) for r in results] + [dma((2, 6))],
        )(*results)
        return y, dx, dmix, jnp.swapaxes(dg_t, 2, 3), jnp.swapaxes(du_t, 2, 3), dw

    return jax.shard_map(device_step, mesh=mesh,
                         in_specs=(tok_spec, tok_spec, route_spec, route_spec, whole_spec,
                                   expert_spec, expert_spec, expert_spec),
                         out_specs=(tok_spec, tok_spec, whole_spec, expert_spec, expert_spec, expert_spec),
                         check_vma=False)
```

```python
import functools

import jax
import jax.numpy as jnp
from jax import lax
from jax.experimental import pallas as pl
from jax.experimental.pallas import tpu as pltpu
from jax.sharding import PartitionSpec as P

NZ, NY, NX = 8, 4, 4
T = 32
D = 512
FF, FP = 352, 384
GR = 3 * FF
HR = GR // 2
NEP, NDP = NZ * NY, 2 * NX
NT = NEP * T
CH = NY * T
SL = D // NEP
BF, F32 = jnp.bfloat16, jnp.float32
MESH = pl.DeviceIdType.MESH
PLUS, MINUS = 0, 1
SIGN = (1, -1)
LANES = 128
ZSEM = (2, 4, 4)


def vmem(dims, dtype=BF):
    return pltpu.VMEM(dims, dtype)


def both(*dims):
    return (2, 2, *dims)


def dot(a, b, ca=1, cb=0):
    return lax.dot_general(a, b, (((ca,), (cb,)), ((), ())), preferred_element_type=F32)


def dot_nt(a, b):
    return dot(a, b, 1, 1)


def dot_tn(a, b):
    return dot(a, b, 0, 0)


def lim(direction, unit):
    return 4 if (unit < 2) == (direction == PLUS) else 3


def step_kernel(tok, dout, ids, gates, wmix, wg_hbm, wu_hbm, wd_hbm,
                y_out, dx_out, dmix_out, dg_out, du_out, dw_out,
                w3, x1, x2, dyg, du2, du1, u1, u2, gt, ab, hb, dab, cb_, pacc, pacc2,
                rs_first, rs_recv, rs_fin, rs_ys, rs_yr,
                grad, rd, rg, fin,
                dm_full, dm_own, dm_send, dm_recv, dm_all, dm_part, dm_mid, dm_y, dm_z,
                w_sem, ag_ys, ag_yr, ag_zs, ag_zr, rs_s, rs_r, rs_ysm, rs_yrm,
                ar_s, ar_r, dx_s, dx_r, out_sem, dy_s, dy_r,
                mg_s, mg_r, ms_s, ms_r):
    ep = lax.axis_index('ep')
    dp = lax.axis_index('dp')
    z, y = lax.div(ep, NY), lax.rem(ep, NY)
    x, core = lax.div(dp, 2), lax.rem(dp, 2)

    z_at = [lax.rem(z + i, NZ) for i in range(NZ)]
    y_at = [lax.rem(y + i, NY) for i in range(NY)]
    x_at = [lax.rem(x + i, NX) for i in range(NX)]
    ep_at = [[zz * NY + yy for yy in y_at] for zz in z_at]
    rows_at = {rows: [[pl.multiple_of(v * rows, rows) for v in line] for line in ep_at] for rows in (T, SL)}
    plane_at = [zz * NY for zz in z_at]
    home_at = [[pl.multiple_of((zz + yd) * T, T) for yd in range(NY)] for zz in plane_at]
    unit_at = [pl.multiple_of(yy * T, T) for yy in y_at]
    dp_x = [xx * 2 + core for xx in x_at]
    dp_r = [lax.rem(dp + r, 8) for r in range(8)]
    partner = dp + 1 - 2 * core
    q128 = [pl.multiple_of(xx * 128, 128) for xx in x_at]
    q64 = [[pl.multiple_of(xx * 128 + 64 * h, 64) for h in range(2)] for xx in x_at]

    def ep_of(dz, dy):
        return ep_at[dz % NZ][dy % NY]

    def dp_of(dx):
        return dp_x[dx % NX]

    def remote(src, dst, ssem, rsem, ep_to=None, dp_to=None):
        return pltpu.make_async_remote_copy(
            src_ref=src, dst_ref=dst, send_sem=ssem, recv_sem=rsem,
            device_id=(ep if ep_to is None else ep_to, dp if dp_to is None else dp_to),
            device_id_type=MESH)

    barrier = pltpu.get_barrier_semaphore()

    @pl.loop(1, NEP)
    def _(r):
        pl.semaphore_signal(barrier, inc=1, device_id=(lax.rem(ep + r, NEP), dp), device_id_type=MESH)

    for r in range(1, NDP):
        pl.semaphore_signal(barrier, inc=1, device_id=(ep, dp_r[r]), device_id_type=MESH)

    loads = []
    for p, src in enumerate((wg_hbm, wu_hbm, wd_hbm)):
        for l in range(2):
            for e in range(2):
                loads.append(pltpu.make_async_copy(src.at[l, e], w3.at[l, e, pl.ds(FP * p, FF), :],
                                                   w_sem.at[p, l, e]))
    for load in loads:
        load.start()

    class Gather:
        def __init__(self, view, s, r):
            self.view, self.s, self.r = view, s, r

        def block(self, dz, dy):
            return self.view(dz % NZ, dy % NY)

        def ycopy(self, j, from_j):
            blk = self.block(0, -from_j)
            return remote(blk, blk, ag_ys.at[self.s, j - 1], ag_yr.at[self.r, j - 1], ep_to=ep_of(0, j))

        def zcopy(self, direction, dist, j, arriving):
            sign = SIGN[direction]
            blk = self.block(-sign * (dist if arriving else dist - 1), -j)
            return remote(blk, blk, ag_zs.at[self.s, direction, dist - 1, j],
                          ag_zr.at[self.r, direction, dist - 1, j], ep_to=ep_of(sign, 0))

        def start(self):
            for direction in (PLUS, MINUS):
                self.zcopy(direction, 1, 0, False).start()
            for j in range(1, NY):
                self.ycopy(j, 0).start()

        def y_arrive(self):
            for j in (1, 3, 2):
                self.ycopy(j, j).wait_recv()
                for direction in (PLUS, MINUS):
                    self.zcopy(direction, 1, j, False).start()

        def poll(self, p):
            dist = p // 2 + 1
            for j in (2 * (p % 2), 2 * (p % 2) + 1):
                for direction in (PLUS, MINUS):
                    if dist <= lim(direction, j):
                        self.zcopy(direction, dist, j, True).wait_recv()
                        if dist < lim(direction, j):
                            self.zcopy(direction, dist + 1, j, False).start()

        def chunk(self, k):
            if k == 0:
                self.y_arrive()
            elif k == 1:
                self.poll(0)
            if k > 0:
                self.poll(k)

        def drain(self):
            for j in range(1, NY):
                self.ycopy(j, 0).wait_send()
            for direction in (PLUS, MINUS):
                for j in range(NY):
                    for dist in range(1, lim(direction, j) + 1):
                        self.zcopy(direction, dist, j, False).wait_send()

    class ColumnGather:
        def zcopy(self, direction, dist, arriving):
            sign = SIGN[direction]
            zz = z_at[(-sign * (dist if arriving else dist - 1)) % NZ]
            blk = dyg.at[zz, pl.ds(unit_at[0], T), :]
            return remote(blk, blk, dy_s.at[direction, dist - 1], dy_r.at[direction, dist - 1], ep_to=ep_of(sign, 0))

        def ycopy(self, direction, hop, arriving):
            sign = SIGN[direction]
            col = unit_at[(-sign * (hop if arriving else hop - 1)) % NY]
            planes = pl.ds(0, NZ) if hop == 1 else pl.ds(4 * direction, 4)
            blk = dyg.at[planes, pl.ds(col, T), :]
            return remote(blk, blk, dy_s.at[direction, 3 + hop], dy_r.at[direction, 3 + hop], ep_to=ep_of(0, sign))

        def start(self):
            for direction in (PLUS, MINUS):
                self.zcopy(direction, 1, False).start()

        def zpoll(self, dist):
            for direction in (PLUS, MINUS):
                if dist <= 4 - direction:
                    self.zcopy(direction, dist, True).wait_recv()
                    if dist < 4 - direction:
                        self.zcopy(direction, dist + 1, False).start()
            if dist == 4:
                for direction in (PLUS, MINUS):
                    self.ycopy(direction, 1, False).start()

        def ypoll(self, hop):
            for direction in (PLUS, MINUS):
                self.ycopy(direction, hop, True).wait_recv()
                if hop == 1:
                    self.ycopy(direction, 2, False).start()

        def drain(self):
            for direction in (PLUS, MINUS):
                for dist in range(1, 5 - direction):
                    self.zcopy(direction, dist, False).wait_send()
                for hop in (1, 2):
                    self.ycopy(direction, hop, False).wait_send()

    class Scatter:
        def __init__(self, part, n):
            self.part, self.n = part, n

        def rows(self, dz, yd):
            return pl.ds(home_at[dz % NZ][yd], T)

        def zcopy(self, direction, s, yd):
            sign = SIGN[direction]
            unit = pl.ds(yd * T, T)
            n = self.n
            src = rs_first.at[n, direction, unit, :] if s == 0 else rs_recv.at[n, direction, s - 1, unit, :]
            last = s == lim(direction, yd) - 1
            dst = rs_fin.at[n, direction, unit, :] if last else rs_recv.at[n, direction, s, unit, :]
            return remote(src, dst, rs_s.at[n // 3, direction, s, yd], rs_r.at[n, direction, s, yd], ep_to=ep_of(sign, 0))

        def round(self, s):
            for yd in range(NY):
                for direction in (PLUS, MINUS):
                    hops = lim(direction, yd)
                    sign = SIGN[direction]
                    if s > hops:
                        continue
                    if s > 0:
                        self.zcopy(direction, s - 1, yd).wait_recv()
                    if s == hops:
                        continue
                    unit = pl.ds(yd * T, T)
                    mine = self.part[self.rows(sign * (hops - s), yd), :]
                    if s == 0:
                        rs_first[self.n, direction, unit, :] = mine.astype(BF)
                    else:
                        got = rs_recv[self.n, direction, s - 1, unit, :]
                        rs_recv[self.n, direction, s - 1, unit, :] = (mine + got.astype(F32)).astype(BF)
                    self.zcopy(direction, s, yd).start()

        def plane(self, dy):
            unit = pl.ds(unit_at[dy % NY], T)
            return (self.part[pl.ds(rows_at[T][0][dy % NY], T), :] + rs_fin[self.n, PLUS, unit, :].astype(F32)
                    + rs_fin[self.n, MINUS, unit, :].astype(F32))

        def ycopy(self, j):
            return remote(rs_ys.at[self.n, j - 1], rs_yr.at[self.n, j - 1], rs_ysm.at[self.n // 3, j - 1],
                          rs_yrm.at[self.n, j - 1], ep_to=ep_of(0, j))

        def y_start(self):
            for j in range(1, NY):
                rs_ys[self.n, j - 1] = self.plane(j).astype(BF)
                self.ycopy(j).start()

        def finish(self):
            total = self.plane(0)
            for j in range(1, NY):
                self.ycopy(j).wait_recv()
                total = total + rs_yr[self.n, j - 1].astype(F32)
            return total

        def drain(self):
            for yd in range(NY):
                for direction in (PLUS, MINUS):
                    for s in range(lim(direction, yd)):
                        self.zcopy(direction, s, yd).wait_send()
            for j in range(1, NY):
                self.ycopy(j).wait_send()

    class Reduce:
        def __init__(self, n):
            self.n = n

        def copy(self, src, dst, slot, dp_to):
            return remote(src, dst, ar_s.at[self.n, slot], ar_r.at[self.n, slot], dp_to=dp_to)

        def swap(self):
            n = self.n
            return self.copy(grad.at[n, 1 - core, pl.ds(0, GR), :], rd.at[n], 0, partner)

        def part(self, q, h):
            return rd.at[self.n, pl.ds(HR * h, HR), pl.ds(q128[q % NX], LANES)]

        def slot(self, i):
            return rg.at[self.n, i]

        def scatter_copy(self, i):
            right, left = dp_of(1), dp_of(-1)
            src = self.slot(i - 4) if i >= 4 else self.part(*((2, 0), (-2, 1), (-1, 0), (1, 1))[i])
            to = [right, left, left, right, right, left][i]
            return self.copy(src, self.slot(i), 1 + i, to)

        def fin(self, q, h=None):
            rows = pl.ds(0, GR) if h is None else pl.ds(HR * h, HR)
            return fin.at[self.n, core, rows, pl.ds(q128[q % NX], LANES)]

        def gather_copy(self, i, arriving=False):
            right, left = dp_of(1), dp_of(-1)
            sent = [(0,), (0,), (-1, 0), (1, 1)][i]
            came = [(-1,), (1,), (-2, 0), (2, 1)][i]
            ref = self.fin(*(came if arriving else sent))
            return self.copy(ref, ref, 7 + i, [right, left, right, left][i])

        def back(self, arriving=False):
            ref = fin.at[self.n, 1 - core if arriving else core]
            return self.copy(ref, ref, 11, partner)

        def out(self):
            return [pltpu.make_async_copy(fin.at[self.n, e, pl.ds(FF * p, FF), :], dst.at[self.n, e],
                                          out_sem.at[self.n, e, p])
                    for e in range(2) for p, dst in enumerate((dg_out, du_out, dw_out))]

        def stage(self, i):
            n = self.n
            if i == 0:
                self.swap().start()
            elif i == 1:
                self.swap().wait_recv()

                @pl.loop(0, 3)
                def _(r):
                    rows = pl.ds(pl.multiple_of(r * FF, FF), FF)
                    rd[n, rows, :] = (rd[n, rows, :].astype(F32) + grad[n, core, rows, :].astype(F32)).astype(BF)

                for i2 in range(4):
                    self.scatter_copy(i2).start()
            elif i == 2:
                for i2 in range(2):
                    self.scatter_copy(i2).wait_recv()
                    got = self.slot(i2)
                    got[...] = (got[...].astype(F32) + self.part(SIGN[i2], i2)[...].astype(F32)).astype(BF)
                    self.scatter_copy(4 + i2).start()
            elif i == 3:
                for i2 in range(2, 6):
                    self.scatter_copy(i2).wait_recv()
                for h in range(2):
                    self.fin(0, h)[...] = (self.part(0, h)[...].astype(F32) + self.slot(2 + h)[...].astype(F32)
                                           + self.slot(4 + h)[...].astype(F32)).astype(BF)
                self.gather_copy(0).start()
                self.gather_copy(1).start()
            elif i == 4:
                for i2 in range(2):
                    self.gather_copy(i2, True).wait_recv()
                    self.gather_copy(2 + i2).start()
            elif i == 5:
                self.gather_copy(2, True).wait_recv()
                self.gather_copy(3, True).wait_recv()
                self.back().start()
            elif i == 6:
                self.back(True).wait_recv()
                for c in self.out():
                    c.start()
                for i2 in range(6):
                    self.scatter_copy(i2).wait_send()
                for i2 in range(4):
                    self.gather_copy(i2).wait_send()
                self.swap().wait_send()
                self.back().wait_send()
            elif i == 7:
                for c in self.out():
                    c.wait()

    slice_rows = pl.ds(pl.multiple_of(lax.rem(ep, 8) * SL, SL), SL)

    def mix_copy(n, r):
        return remote(dm_send.at[n], dm_recv.at[n, r - 1], dx_s.at[n, r - 1], dx_r.at[n, r - 1], dp_to=dp_r[r])

    def mix_send(n):
        dm_send[n] = dm_own[n].astype(BF)
        for r in range(1, NDP):
            mix_copy(n, r).start()

    def mix_start(n, xg, dug):
        lanes = pl.ds(pl.multiple_of(lax.div(ep, 8) * LANES, LANES), LANES)
        dm_full[...] = dot_tn(xg[:, lanes], dug[...])
        dm_own[n] = dm_full[slice_rows, :]
        mix_send(n)

    def mix_sum(n):
        total = dm_own[n]
        for r in range(1, NDP):
            mix_copy(n, r).wait_recv()
            total = total + dm_recv[n, r - 1].astype(F32)
        dm_all[n, own_slice, :] = total.astype(BF)
        for r in range(1, NDP):
            mix_copy(n, r).wait_send()

    def half_at(half):
        return pl.ds(pl.multiple_of(half * (D // 2), D // 2), D // 2)

    def slice_at(place):
        return pl.ds(pl.multiple_of(place * SL, SL), SL)

    def mix_gather_copy(n, r, place):
        blk = dm_all.at[n, slice_at(place), half_at(core)]
        return remote(blk, blk, mg_s.at[n, r], mg_r.at[n, r], ep_to=lax.rem(ep + r, NEP))

    def mix_swap(n, half):
        blk = dm_all.at[n, :, half_at(half)]
        return remote(blk, blk, mg_s.at[n, 0], mg_r.at[n, 0], dp_to=partner)

    def mix_gather_start(n):
        @pl.loop(1, NEP)
        def _(r):
            mix_gather_copy(n, r, ep).start()

    def mix_gather_done(n):
        @pl.loop(1, NEP)
        def _(r):
            mix_gather_copy(n, r, lax.rem(ep + NEP - r, NEP)).wait_recv()
            mix_gather_copy(n, r, ep).wait_send()

        mix_swap(n, core).start()

    def mix_swap_done(n):
        mix_swap(n, 1 - core).wait_recv()
        mix_swap(n, core).wait_send()

    def mix_y_copy(j):
        return remote(dm_part.at[:, unit_slice[j], :], dm_y.at[j - 1], ms_s.at[j], ms_r.at[j], ep_to=ep_of(0, j))

    def mix_z_copy(i):
        return remote(dm_mid.at[z_at[i]], dm_z.at[i - 1], ms_s.at[NY + i], ms_r.at[NY + i], ep_to=ep_of(i, 0))

    def mix_scatter_start():
        @pl.loop(0, NZ)
        def _(i):
            rows = pl.ds(pl.multiple_of(i * CH, CH), CH)
            du1[rows, :] = pacc[rows, :].astype(BF)

        du1[own_rows, :] = (pacc[own_rows, :] + dyg[z, home_unit, :].astype(F32)).astype(BF)

        @pl.loop(0, 4)
        def _(i):
            rows = pl.ds(pl.multiple_of(i * LANES, LANES), LANES)
            both_planes = dot_tn(x1[:, rows], du1[...]).astype(BF)
            half = LANES // 2
            dm_part[2 * i] = both_planes[:half]
            dm_part[2 * i + 1] = both_planes[half:]

        for j in range(1, NY):
            mix_y_copy(j).start()

    def mix_scatter_turn():
        for j in range(1, NY):
            mix_y_copy(j).wait_recv()

        @pl.loop(0, NZ)
        def _(i):
            total = dm_part[i, unit_slice[0], :].astype(F32)
            for j in range(1, NY):
                total = total + dm_y[j - 1, i].astype(F32)
            dm_mid[i] = total.astype(BF)

        for i in range(1, NZ):
            mix_z_copy(i).start()

    def mix_scatter_sum():
        total = dm_mid[z].astype(F32)
        for i in range(1, NZ):
            mix_z_copy(i).wait_recv()
            total = total + dm_z[i - 1].astype(F32)
        dm_own[0] = total
        mix_send(0)

    def mix_scatter_drain():
        for j in range(1, NY):
            mix_y_copy(j).wait_send()
        for i in range(1, NZ):
            mix_z_copy(i).wait_send()

    unit_slice = [pl.ds(pl.multiple_of(yy * SL, SL), SL) for yy in y_at]
    own_slice = slice_at(ep)
    own_rows = pl.ds(rows_at[T][0][0], T)
    home_unit = pl.ds(unit_at[0], T)

    def plane_rows(k):
        return pl.ds(pl.multiple_of(plane_of(k) * CH, CH), CH)

    def plane_of(k):
        odd = lax.rem(k, 2)
        dist = lax.div(k + 1, 2)
        return lax.rem(z + NZ - odd * dist + (1 - odd) * dist, NZ)

    def gate_col(layer, e, rows):
        table = gt[rows, :]
        lane = lax.broadcasted_iota(jnp.int32, (CH, 128), 1)
        return jnp.sum(jnp.where(lane == layer * 64 + ep * 2 + e, table, 0.0), axis=1, keepdims=True)

    def expert_in(u, gcol):
        return jnp.where(gcol > 0.0, u, 0.0).astype(BF)

    x1[own_rows, :] = tok[...]
    slot = lax.broadcasted_iota(jnp.int32, (LANES, T), 0)
    table = jnp.zeros((LANES, T), F32)
    for l in range(2):
        for j in range(6):
            table = table + jnp.where(slot == ids[j, l:l + 1, :] + 64 * l, gates[j, l:l + 1, :], 0.0)
    gt[own_rows, :] = table.T
    dyg[z, home_unit, :] = dout[...]
    pl.semaphore_wait(barrier, NEP + NDP - 2)

    def row_view(buf):
        return lambda dz, dy: buf.at[pl.ds(rows_at[T][dz][dy], T), :]

    ag_tok = Gather(row_view(x1), 0, 0)
    ag_gt = Gather(row_view(gt), 1, 1)
    ag_dy = ColumnGather()
    ag_x2 = Gather(row_view(x2), 0, 2)
    ag_du2 = Gather(row_view(du2), 1, 3)
    ag_tok.start()
    ag_gt.start()
    ag_dy.start()

    for load in loads:
        load.wait()
    for l in range(2):
        for e in range(2):
            for p in range(3):
                w3[l, e, FP * p + FF:FP * p + FP, :] = jnp.zeros((FP - FF, D), BF)

    def gate_up(l, e):
        return w3[l, e, 0:2 * FP, :]

    def down(l, e):
        return w3[l, e, 2 * FP:, :]

    @pl.loop(0, 8)
    def _(k):
        for kk in range(8):
            @pl.when(k == kk)
            def _(kk=kk):
                ag_tok.chunk(kk)
                ag_gt.chunk(kk)
                if kk % 2:
                    ag_dy.zpoll(kk // 2 + 1)
        rows = plane_rows(k)
        xc = x1[rows, :]
        u = (xc.astype(F32) + dot(xc, wmix[0])).astype(BF)
        u1[rows, :] = u
        uf = u.astype(F32)
        total = jnp.zeros((CH, D), F32)
        for e in range(2):
            gcol = gate_col(0, e, rows)
            pre = dot_nt(expert_in(uf, gcol), gate_up(0, e))
            ab[e, rows, :] = pre
            a, b = pre[:, :FP], pre[:, FP:]
            h = (a * jax.nn.sigmoid(a) * b).astype(BF)
            hb[0, e, rows, :] = h
            total = total + gcol * dot(h, down(0, e)).astype(BF).astype(F32)
        pacc[rows, :] = total

    rs = Scatter(pacc, 0)
    for s in range(5):
        rs.round(s)
        if s in (2, 4):
            ag_dy.ypoll(s // 2)
    rs.y_start()
    ag_tok.drain()
    ag_gt.drain()
    ag_dy.drain()
    y1 = (u1[own_rows, :].astype(F32) + rs.finish()).astype(BF)
    x2[own_rows, :] = y1
    ag_x2.start()
    rs.drain()

    def backward_part(layer, e, rows, gcol, dyc, pre):
        a, b = pre[:, :FP], pre[:, FP:]
        c = (gcol * dyc).astype(BF)
        cb_[e, rows, :] = c
        dh = dot_nt(c, down(layer, e))
        s = jax.nn.sigmoid(a)
        dab[e, rows, 0:FP] = (dh * b * (s * (1.0 + a * (1.0 - s)))).astype(BF)
        dab[e, rows, FP:] = (dh * (a * s)).astype(BF)
        v = dot(dab[e, rows, :], gate_up(layer, e)).astype(BF)
        return gcol * v.astype(F32)

    @pl.loop(0, 8)
    def _(k):
        for kk in range(8):
            @pl.when(k == kk)
            def _(kk=kk):
                ag_x2.chunk(kk)
        rows = plane_rows(k)
        xc = x2[rows, :]
        u = (xc.astype(F32) + dot(xc, wmix[1])).astype(BF)
        u2[rows, :] = u
        uf = u.astype(F32)
        dyc = dyg[plane_of(k)].astype(F32)
        total = jnp.zeros((CH, D), F32)
        back = jnp.zeros((CH, D), F32)
        for e in range(2):
            gcol = gate_col(1, e, rows)
            pre = dot_nt(expert_in(uf, gcol), gate_up(1, e))
            a, b = pre[:, :FP], pre[:, FP:]
            h = (a * jax.nn.sigmoid(a) * b).astype(BF)
            hb[1, e, rows, :] = h
            total = total + gcol * dot(h, down(1, e)).astype(BF).astype(F32)
            back = back + backward_part(1, e, rows, gcol, dyc, pre)
        pacc2[rows, :] = total
        pacc[rows, :] = back

    def weight_grads(layer, e, ug):
        @pl.loop(0, 6)
        def _(i):
            part = lax.div(i, 3)
            cols = pl.ds(pl.multiple_of(i * LANES, LANES), LANES)
            rows = pl.ds(pl.multiple_of(part * FF + (i - 3 * part) * LANES, 32), LANES)
            grad[layer, e, rows, :] = dot_tn(dab[e, :, cols], ug[...]).astype(BF)

        @pl.loop(0, 3)
        def _(i):
            cols = pl.ds(pl.multiple_of(i * LANES, LANES), LANES)
            rows = pl.ds(pl.multiple_of(2 * FF + i * LANES, 32), LANES)
            grad[layer, e, rows, :] = dot_tn(hb[layer, e, :, cols], cb_[e]).astype(BF)

    rs = Scatter(pacc, 1)
    rs.round(0)
    weight_grads(1, 1 - core, u2)
    ar2 = Reduce(1)
    ar2.stage(0)
    rs.round(1)
    weight_grads(1, core, u2)
    rs.round(2)
    ar2.stage(1)
    for s in range(3, 5):
        rs.round(s)
    rs.y_start()
    ag_x2.drain()
    du2[own_rows, :] = (dout[...].astype(F32) + rs.finish()).astype(BF)
    ag_du2.start()
    rs.drain()

    @pl.loop(0, 8)
    def _(k):
        for kk in range(8):
            @pl.when(k == kk)
            def _(kk=kk):
                ag_du2.chunk(kk)
                if kk == 1:
                    ar2.stage(2)
                if kk == 4:
                    ar2.stage(3)
                if kk == 7:
                    ar2.stage(4)
        rows = plane_rows(k)
        duc = du2[rows, :]
        dyc = (duc.astype(F32) + dot_nt(duc, wmix[1])).astype(BF)
        dyg[plane_of(k)] = dyc
        dyc = dyc.astype(F32)
        back = jnp.zeros((CH, D), F32)
        for e in range(2):
            back = back + backward_part(0, e, rows, gate_col(0, e, rows), dyc, ab[e, rows, :])
        pacc[rows, :] = back

    rs = Scatter(pacc, 2)
    rs_y2 = Scatter(pacc2, 3)
    rs.round(0)
    weight_grads(0, 1 - core, u1)
    ar1 = Reduce(0)
    ar1.stage(0)
    mix_scatter_start()
    rs.round(1)
    mix_start(1, x2, du2)
    weight_grads(0, core, u1)
    ar1.stage(1)
    rs.round(2)
    mix_sum(1)
    ar2.stage(5)
    rs.round(3)
    mix_scatter_turn()
    rs.round(4)
    rs.y_start()
    ar1.stage(2)
    rs_y2.round(0)
    ar2.stage(6)
    d_u1 = (dyg[z, home_unit, :].astype(F32) + rs.finish()).astype(BF)
    dx_out[...] = (d_u1.astype(F32) + dot_nt(d_u1, wmix[0])).astype(BF)
    mix_scatter_sum()
    rs_y2.round(1)
    mix_gather_start(1)
    ar1.stage(3)
    rs_y2.round(2)
    mix_sum(0)
    mix_gather_start(0)
    rs_y2.round(3)
    ar1.stage(4)
    rs_y2.round(4)
    rs_y2.y_start()
    ar2.stage(7)
    ag_du2.drain()
    rs.drain()
    mix_scatter_drain()
    mix_gather_done(1)
    ar1.stage(5)
    y_out[...] = (u2[own_rows, :].astype(F32) + rs_y2.finish()).astype(BF)
    mix_swap_done(1)
    dmix_out[1] = dm_all[1]
    mix_gather_done(0)
    ar1.stage(6)
    mix_swap_done(0)
    dmix_out[0] = dm_all[0]
    rs_y2.drain()
    ar1.stage(7)


def copy_kernel(*refs):
    n = len(refs) // 3
    src, dst, buf, sem = refs[:n], refs[n:2 * n], refs[2 * n:3 * n], refs[3 * n]
    loads = [pltpu.make_async_copy(src[i], buf[i], sem.at[0, i]) for i in range(n)]
    stores = [pltpu.make_async_copy(buf[i], dst[i], sem.at[1, i]) for i in range(n)]
    for load in loads:
        load.start()
    for load, store in zip(loads, stores):
        load.wait()
        store.start()
    for store in stores:
        store.wait()


def solution(mesh):
    tok_spec = P(('dp', 'ep'))
    route_spec = P(None, ('dp', 'ep'))
    whole_spec = P()
    expert_spec = P(None, 'ep')

    def device_step(tokens, d_out, expert_ids, gate_vals, w_mix, w_gate, w_up, w_down):
        vm = pl.BlockSpec(memory_space=pltpu.VMEM)
        hbm = pl.BlockSpec(memory_space=pl.ANY)
        shape = jax.ShapeDtypeStruct
        dma = pltpu.SemaphoreType.DMA
        wg_t, wu_t = jnp.swapaxes(w_gate, 2, 3), jnp.swapaxes(w_up, 2, 3)
        results = pl.pallas_call(
            step_kernel,
            out_shape=(shape((T, D), BF), shape((T, D), BF), shape((2, D, D), BF),
                       *[shape(both(FF, D), BF)] * 3),
            in_specs=[vm] * 5 + [hbm] * 3,
            out_specs=(vm,) * 3 + (hbm,) * 3,
            scratch_shapes=[
                vmem(both(3 * FP, D)),
                *[vmem((NT, D))] * 2, vmem((NZ, CH, D)), *[vmem((NT, D))] * 4,
                vmem((NT, LANES), F32), vmem((2, NT, 2 * FP), F32),
                vmem(both(NT, FP)), vmem((2, NT, 2 * FP)), vmem((2, NT, D)),
                vmem((NT, D), F32), vmem((NT, D), F32),
                vmem((4, 2, CH, D)), vmem((4, 2, 3, CH, D)), vmem((4, 2, CH, D)),
                vmem((4, 3, T, D)), vmem((4, 3, T, D)),
                vmem(both(GR + 32, D)), vmem((2, GR, D)), vmem((2, 6, HR, LANES)), vmem(both(GR, D)),
                vmem((LANES, D), F32), vmem((2, SL, D), F32), vmem((2, SL, D)), vmem((2, 7, SL, D)),
                vmem((2, D, D)), vmem((NZ, NY * SL, D)), vmem((NZ, SL, D)),
                vmem((NY, NZ, SL, D)), vmem((NZ, SL, D)),
                dma((3, 2, 2)),
                dma((2, 3)), dma((4, 3)), dma((2, *ZSEM)), dma((4, *ZSEM)),
                dma((2, *ZSEM)), dma((4, *ZSEM)), dma((2, 3)), dma((4, 3)),
                *[dma((2, 12))] * 2, *[dma((2, 7))] * 2, dma((2, 2, 3)), *[dma((2, 6))] * 2,
                *[dma((2, NEP))] * 2, *[dma((NEP,))] * 2,
            ],
            compiler_params=pltpu.CompilerParams(
                collective_id=0, has_side_effects=True, vmem_limit_bytes=67043328),
        )(tokens, d_out, jnp.transpose(expert_ids, (2, 0, 1)), jnp.transpose(gate_vals, (2, 0, 1)),
          w_mix, wg_t, wu_t, w_down)
        y, dx, dmix, dg_t, du_t, dw = pl.pallas_call(
            copy_kernel,
            out_shape=[shape(r.shape, r.dtype) for r in results],
            in_specs=[hbm] * 6,
            out_specs=[hbm] * 6,
            scratch_shapes=[vmem(r.shape) for r in results] + [dma((2, 6))],
        )(*results)
        return y, dx, dmix, jnp.swapaxes(dg_t, 2, 3), jnp.swapaxes(du_t, 2, 3), dw

    return jax.shard_map(device_step, mesh=mesh,
                         in_specs=(tok_spec, tok_spec, route_spec, route_spec, whole_spec,
                                   expert_spec, expert_spec, expert_spec),
                         out_specs=(tok_spec, tok_spec, whole_spec, expert_spec, expert_spec, expert_spec),
                         check_vma=False)
```

```python
import functools

import jax
import jax.numpy as jnp
from jax import lax
from jax.experimental import pallas as pl
from jax.experimental.pallas import tpu as pltpu
from jax.sharding import PartitionSpec as P

NZ, NY, NX = 8, 4, 4
T = 32
D = 512
FF, FP = 352, 384
GR = 3 * FF
HR = GR // 2
NEP, NDP = NZ * NY, 2 * NX
NT = NEP * T
CH = NY * T
SL = D // NEP
BF, F32 = jnp.bfloat16, jnp.float32
MESH = pl.DeviceIdType.MESH
PLUS, MINUS = 0, 1
SIGN = (1, -1)
LANES = 128
ZSEM = (2, 4, 4)


def vmem(dims, dtype=BF):
    return pltpu.VMEM(dims, dtype)


def both(*dims):
    return (2, 2, *dims)


def dot(a, b, ca=1, cb=0):
    return lax.dot_general(a, b, (((ca,), (cb,)), ((), ())), preferred_element_type=F32)


def dot_nt(a, b):
    return dot(a, b, 1, 1)


def dot_tn(a, b):
    return dot(a, b, 0, 0)


def lim(direction, unit):
    return 4 if (unit < 2) == (direction == PLUS) else 3


def step_kernel(tok, dout, ids, gates, wmix, wg_hbm, wu_hbm, wd_hbm,
                y_out, dx_out, dmix_out, dg_out, du_out, dw_out,
                w3, x1, x2, dyg, du2, du1, u1, u2, gt, ab, hb, dab, cb_, pacc, pacc2,
                rs_first, rs_recv, rs_fin, rs_ys, rs_yr,
                grad, rd, rg, fin,
                dm_full, dm_own, dm_send, dm_recv, dm_all, dm_part, dm_mid, dm_y, dm_z,
                w_sem, ag_ys, ag_yr, ag_zs, ag_zr, rs_s, rs_r, rs_ysm, rs_yrm,
                ar_s, ar_r, dx_s, dx_r, out_sem, dy_s, dy_r,
                mg_s, mg_r, ms_s, ms_r):
    ep = lax.axis_index('ep')
    dp = lax.axis_index('dp')
    z, y = lax.div(ep, NY), lax.rem(ep, NY)
    x, core = lax.div(dp, 2), lax.rem(dp, 2)

    z_at = [lax.rem(z + i, NZ) for i in range(NZ)]
    y_at = [lax.rem(y + i, NY) for i in range(NY)]
    x_at = [lax.rem(x + i, NX) for i in range(NX)]
    ep_at = [[zz * NY + yy for yy in y_at] for zz in z_at]
    rows_at = {rows: [[pl.multiple_of(v * rows, rows) for v in line] for line in ep_at] for rows in (T, SL)}
    plane_at = [zz * NY for zz in z_at]
    home_at = [[pl.multiple_of((zz + yd) * T, T) for yd in range(NY)] for zz in plane_at]
    unit_at = [pl.multiple_of(yy * T, T) for yy in y_at]
    dp_x = [xx * 2 + core for xx in x_at]
    dp_r = [lax.rem(dp + r, 8) for r in range(8)]
    partner = dp + 1 - 2 * core
    q128 = [pl.multiple_of(xx * 128, 128) for xx in x_at]
    q64 = [[pl.multiple_of(xx * 128 + 64 * h, 64) for h in range(2)] for xx in x_at]

    def ep_of(dz, dy):
        return ep_at[dz % NZ][dy % NY]

    def dp_of(dx):
        return dp_x[dx % NX]

    def remote(src, dst, ssem, rsem, ep_to=None, dp_to=None):
        return pltpu.make_async_remote_copy(
            src_ref=src, dst_ref=dst, send_sem=ssem, recv_sem=rsem,
            device_id=(ep if ep_to is None else ep_to, dp if dp_to is None else dp_to),
            device_id_type=MESH)

    barrier = pltpu.get_barrier_semaphore()
    peers = [(ep_of(0, j), dp) for j in range(1, NY)] + [(ep_of(sign, 0), dp) for sign in SIGN]
    peers += [(ep, place) for place in dp_r[1:]]
    for peer in peers:
        pl.semaphore_signal(barrier, inc=1, device_id=peer, device_id_type=MESH)

    loads = []
    for p, src in enumerate((wg_hbm, wu_hbm, wd_hbm)):
        for l in range(2):
            for e in range(2):
                loads.append(pltpu.make_async_copy(src.at[l, e], w3.at[l, e, pl.ds(FP * p, FF), :],
                                                   w_sem.at[p, l, e]))
    for load in loads:
        load.start()

    class Gather:
        def __init__(self, view, s, r):
            self.view, self.s, self.r = view, s, r

        def block(self, dz, dy):
            return self.view(dz % NZ, dy % NY)

        def ycopy(self, j, from_j):
            blk = self.block(0, -from_j)
            return remote(blk, blk, ag_ys.at[self.s, j - 1], ag_yr.at[self.r, j - 1], ep_to=ep_of(0, j))

        def zcopy(self, direction, dist, j, arriving):
            sign = SIGN[direction]
            blk = self.block(-sign * (dist if arriving else dist - 1), -j)
            return remote(blk, blk, ag_zs.at[self.s, direction, dist - 1, j],
                          ag_zr.at[self.r, direction, dist - 1, j], ep_to=ep_of(sign, 0))

        def start(self):
            for direction in (PLUS, MINUS):
                self.zcopy(direction, 1, 0, False).start()
            for j in range(1, NY):
                self.ycopy(j, 0).start()

        def y_arrive(self):
            for j in (1, 3, 2):
                self.ycopy(j, j).wait_recv()
                for direction in (PLUS, MINUS):
                    self.zcopy(direction, 1, j, False).start()

        def poll(self, p):
            dist = p // 2 + 1
            for j in (2 * (p % 2), 2 * (p % 2) + 1):
                for direction in (PLUS, MINUS):
                    if dist <= lim(direction, j):
                        self.zcopy(direction, dist, j, True).wait_recv()
                        if dist < lim(direction, j):
                            self.zcopy(direction, dist + 1, j, False).start()

        def chunk(self, k):
            if k == 0:
                self.y_arrive()
            elif k == 1:
                self.poll(0)
            if k > 0:
                self.poll(k)

        def drain(self):
            for j in range(1, NY):
                self.ycopy(j, 0).wait_send()
            for direction in (PLUS, MINUS):
                for j in range(NY):
                    for dist in range(1, lim(direction, j) + 1):
                        self.zcopy(direction, dist, j, False).wait_send()

    class ColumnGather:
        def zcopy(self, direction, dist, arriving):
            sign = SIGN[direction]
            zz = z_at[(-sign * (dist if arriving else dist - 1)) % NZ]
            blk = dyg.at[zz, pl.ds(unit_at[0], T), :]
            return remote(blk, blk, dy_s.at[direction, dist - 1], dy_r.at[direction, dist - 1], ep_to=ep_of(sign, 0))

        def ycopy(self, direction, hop, arriving):
            sign = SIGN[direction]
            col = unit_at[(-sign * (hop if arriving else hop - 1)) % NY]
            planes = pl.ds(0, NZ) if hop == 1 else pl.ds(4 * direction, 4)
            blk = dyg.at[planes, pl.ds(col, T), :]
            return remote(blk, blk, dy_s.at[direction, 3 + hop], dy_r.at[direction, 3 + hop], ep_to=ep_of(0, sign))

        def start(self):
            for direction in (PLUS, MINUS):
                self.zcopy(direction, 1, False).start()

        def zpoll(self, dist):
            for direction in (PLUS, MINUS):
                if dist <= 4 - direction:
                    self.zcopy(direction, dist, True).wait_recv()
                    if dist < 4 - direction:
                        self.zcopy(direction, dist + 1, False).start()
            if dist == 4:
                for direction in (PLUS, MINUS):
                    self.ycopy(direction, 1, False).start()

        def ypoll(self, hop):
            for direction in (PLUS, MINUS):
                self.ycopy(direction, hop, True).wait_recv()
                if hop == 1:
                    self.ycopy(direction, 2, False).start()

        def drain(self):
            for direction in (PLUS, MINUS):
                for dist in range(1, 5 - direction):
                    self.zcopy(direction, dist, False).wait_send()
                for hop in (1, 2):
                    self.ycopy(direction, hop, False).wait_send()

    class Scatter:
        def __init__(self, part, n):
            self.part, self.n = part, n

        def rows(self, dz, yd):
            return pl.ds(home_at[dz % NZ][yd], T)

        def zcopy(self, direction, s, yd):
            sign = SIGN[direction]
            unit = pl.ds(yd * T, T)
            n = self.n
            src = rs_first.at[n, direction, unit, :] if s == 0 else rs_recv.at[n, direction, s - 1, unit, :]
            last = s == lim(direction, yd) - 1
            dst = rs_fin.at[n, direction, unit, :] if last else rs_recv.at[n, direction, s, unit, :]
            return remote(src, dst, rs_s.at[n // 3, direction, s, yd], rs_r.at[n, direction, s, yd], ep_to=ep_of(sign, 0))

        def round(self, s):
            for yd in range(NY):
                for direction in (PLUS, MINUS):
                    hops = lim(direction, yd)
                    sign = SIGN[direction]
                    if s > hops:
                        continue
                    if s > 0:
                        self.zcopy(direction, s - 1, yd).wait_recv()
                    if s == hops:
                        continue
                    unit = pl.ds(yd * T, T)
                    mine = self.part[self.rows(sign * (hops - s), yd), :]
                    if s == 0:
                        rs_first[self.n, direction, unit, :] = mine.astype(BF)
                    else:
                        got = rs_recv[self.n, direction, s - 1, unit, :]
                        rs_recv[self.n, direction, s - 1, unit, :] = (mine + got.astype(F32)).astype(BF)
                    self.zcopy(direction, s, yd).start()

        def plane(self, dy):
            unit = pl.ds(unit_at[dy % NY], T)
            return (self.part[pl.ds(rows_at[T][0][dy % NY], T), :] + rs_fin[self.n, PLUS, unit, :].astype(F32)
                    + rs_fin[self.n, MINUS, unit, :].astype(F32))

        def ycopy(self, j):
            return remote(rs_ys.at[self.n, j - 1], rs_yr.at[self.n, j - 1], rs_ysm.at[self.n // 3, j - 1],
                          rs_yrm.at[self.n, j - 1], ep_to=ep_of(0, j))

        def y_start(self):
            for j in range(1, NY):
                rs_ys[self.n, j - 1] = self.plane(j).astype(BF)
                self.ycopy(j).start()

        def finish(self):
            total = self.plane(0)
            for j in range(1, NY):
                self.ycopy(j).wait_recv()
                total = total + rs_yr[self.n, j - 1].astype(F32)
            return total

        def drain(self):
            for yd in range(NY):
                for direction in (PLUS, MINUS):
                    for s in range(lim(direction, yd)):
                        self.zcopy(direction, s, yd).wait_send()
            for j in range(1, NY):
                self.ycopy(j).wait_send()

    class Reduce:
        def __init__(self, n):
            self.n = n

        def copy(self, src, dst, slot, dp_to):
            return remote(src, dst, ar_s.at[self.n, slot], ar_r.at[self.n, slot], dp_to=dp_to)

        def swap(self):
            n = self.n
            return self.copy(grad.at[n, 1 - core, pl.ds(0, GR), :], rd.at[n], 0, partner)

        def part(self, q, h):
            return rd.at[self.n, pl.ds(HR * h, HR), pl.ds(q128[q % NX], LANES)]

        def slot(self, i):
            return rg.at[self.n, i]

        def scatter_copy(self, i):
            right, left = dp_of(1), dp_of(-1)
            src = self.slot(i - 4) if i >= 4 else self.part(*((2, 0), (-2, 1), (-1, 0), (1, 1))[i])
            to = [right, left, left, right, right, left][i]
            return self.copy(src, self.slot(i), 1 + i, to)

        def fin(self, q, h=None):
            rows = pl.ds(0, GR) if h is None else pl.ds(HR * h, HR)
            return fin.at[self.n, core, rows, pl.ds(q128[q % NX], LANES)]

        def gather_copy(self, i, arriving=False):
            right, left = dp_of(1), dp_of(-1)
            sent = [(0,), (0,), (-1, 0), (1, 1)][i]
            came = [(-1,), (1,), (-2, 0), (2, 1)][i]
            ref = self.fin(*(came if arriving else sent))
            return self.copy(ref, ref, 7 + i, [right, left, right, left][i])

        def back(self, arriving=False):
            ref = fin.at[self.n, 1 - core if arriving else core]
            return self.copy(ref, ref, 11, partner)

        def out(self):
            return [pltpu.make_async_copy(fin.at[self.n, e, pl.ds(FF * p, FF), :], dst.at[self.n, e],
                                          out_sem.at[self.n, e, p])
                    for e in range(2) for p, dst in enumerate((dg_out, du_out, dw_out))]

        def stage(self, i):
            n = self.n
            if i == 0:
                self.swap().start()
            elif i == 1:
                self.swap().wait_recv()

                @pl.loop(0, 3)
                def _(r):
                    rows = pl.ds(pl.multiple_of(r * FF, FF), FF)
                    rd[n, rows, :] = (rd[n, rows, :].astype(F32) + grad[n, core, rows, :].astype(F32)).astype(BF)

                for i2 in range(4):
                    self.scatter_copy(i2).start()
            elif i == 2:
                for i2 in range(2):
                    self.scatter_copy(i2).wait_recv()
                    got = self.slot(i2)
                    got[...] = (got[...].astype(F32) + self.part(SIGN[i2], i2)[...].astype(F32)).astype(BF)
                    self.scatter_copy(4 + i2).start()
            elif i == 3:
                for i2 in range(2, 6):
                    self.scatter_copy(i2).wait_recv()
                for h in range(2):
                    self.fin(0, h)[...] = (self.part(0, h)[...].astype(F32) + self.slot(2 + h)[...].astype(F32)
                                           + self.slot(4 + h)[...].astype(F32)).astype(BF)
                self.gather_copy(0).start()
                self.gather_copy(1).start()
            elif i == 4:
                for i2 in range(2):
                    self.gather_copy(i2, True).wait_recv()
                    self.gather_copy(2 + i2).start()
            elif i == 5:
                self.gather_copy(2, True).wait_recv()
                self.gather_copy(3, True).wait_recv()
                self.back().start()
            elif i == 6:
                self.back(True).wait_recv()
                for c in self.out():
                    c.start()
                for i2 in range(6):
                    self.scatter_copy(i2).wait_send()
                for i2 in range(4):
                    self.gather_copy(i2).wait_send()
                self.swap().wait_send()
                self.back().wait_send()
            elif i == 7:
                for c in self.out():
                    c.wait()

    slice_rows = pl.ds(pl.multiple_of(lax.rem(ep, 8) * SL, SL), SL)

    def mix_copy(n, r):
        return remote(dm_send.at[n], dm_recv.at[n, r - 1], dx_s.at[n, r - 1], dx_r.at[n, r - 1], dp_to=dp_r[r])

    def mix_send(n):
        dm_send[n] = dm_own[n].astype(BF)
        for r in range(1, NDP):
            mix_copy(n, r).start()

    def mix_start(n, xg, dug):
        lanes = pl.ds(pl.multiple_of(lax.div(ep, 8) * LANES, LANES), LANES)
        dm_full[...] = dot_tn(xg[:, lanes], dug[...])
        dm_own[n] = dm_full[slice_rows, :]
        mix_send(n)

    def mix_sum(n):
        total = dm_own[n]
        for r in range(1, NDP):
            mix_copy(n, r).wait_recv()
            total = total + dm_recv[n, r - 1].astype(F32)
        dm_all[n, own_slice, :] = total.astype(BF)
        for r in range(1, NDP):
            mix_copy(n, r).wait_send()

    def half_at(half):
        return pl.ds(pl.multiple_of(half * (D // 2), D // 2), D // 2)

    def slice_at(place):
        return pl.ds(pl.multiple_of(place * SL, SL), SL)

    def mix_gather_copy(n, r, place):
        blk = dm_all.at[n, slice_at(place), half_at(core)]
        return remote(blk, blk, mg_s.at[n, r], mg_r.at[n, r], ep_to=lax.rem(ep + r, NEP))

    def mix_swap(n, half):
        blk = dm_all.at[n, :, half_at(half)]
        return remote(blk, blk, mg_s.at[n, 0], mg_r.at[n, 0], dp_to=partner)

    def mix_gather_start(n):
        @pl.loop(1, NEP)
        def _(r):
            mix_gather_copy(n, r, ep).start()

    def mix_gather_done(n):
        @pl.loop(1, NEP)
        def _(r):
            mix_gather_copy(n, r, lax.rem(ep + NEP - r, NEP)).wait_recv()
            mix_gather_copy(n, r, ep).wait_send()

        mix_swap(n, core).start()

    def mix_swap_done(n):
        mix_swap(n, 1 - core).wait_recv()
        mix_swap(n, core).wait_send()

    def mix_y_copy(j):
        return remote(dm_part.at[:, unit_slice[j], :], dm_y.at[j - 1], ms_s.at[j], ms_r.at[j], ep_to=ep_of(0, j))

    def mix_z_copy(i):
        return remote(dm_mid.at[z_at[i]], dm_z.at[i - 1], ms_s.at[NY + i], ms_r.at[NY + i], ep_to=ep_of(i, 0))

    def mix_scatter_start():
        @pl.loop(0, NZ)
        def _(i):
            rows = pl.ds(pl.multiple_of(i * CH, CH), CH)
            du1[rows, :] = pacc[rows, :].astype(BF)

        du1[own_rows, :] = (pacc[own_rows, :] + dyg[z, home_unit, :].astype(F32)).astype(BF)

        @pl.loop(0, 4)
        def _(i):
            rows = pl.ds(pl.multiple_of(i * LANES, LANES), LANES)
            both_planes = dot_tn(x1[:, rows], du1[...]).astype(BF)
            half = LANES // 2
            dm_part[2 * i] = both_planes[:half]
            dm_part[2 * i + 1] = both_planes[half:]

        for j in range(1, NY):
            mix_y_copy(j).start()

    def mix_scatter_turn():
        for j in range(1, NY):
            mix_y_copy(j).wait_recv()

        @pl.loop(0, NZ)
        def _(i):
            total = dm_part[i, unit_slice[0], :].astype(F32)
            for j in range(1, NY):
                total = total + dm_y[j - 1, i].astype(F32)
            dm_mid[i] = total.astype(BF)

        for i in range(1, NZ):
            mix_z_copy(i).start()

    def mix_scatter_sum():
        total = dm_mid[z].astype(F32)
        for i in range(1, NZ):
            mix_z_copy(i).wait_recv()
            total = total + dm_z[i - 1].astype(F32)
        dm_own[0] = total
        mix_send(0)

    def mix_scatter_drain():
        for j in range(1, NY):
            mix_y_copy(j).wait_send()
        for i in range(1, NZ):
            mix_z_copy(i).wait_send()

    unit_slice = [pl.ds(pl.multiple_of(yy * SL, SL), SL) for yy in y_at]
    own_slice = slice_at(ep)
    own_rows = pl.ds(rows_at[T][0][0], T)
    home_unit = pl.ds(unit_at[0], T)

    def plane_rows(k):
        return pl.ds(pl.multiple_of(plane_of(k) * CH, CH), CH)

    def plane_of(k):
        odd = lax.rem(k, 2)
        dist = lax.div(k + 1, 2)
        return lax.rem(z + NZ - odd * dist + (1 - odd) * dist, NZ)

    def gate_col(layer, e, rows):
        table = gt[rows, :]
        lane = lax.broadcasted_iota(jnp.int32, (CH, 128), 1)
        return jnp.sum(jnp.where(lane == layer * 64 + ep * 2 + e, table, 0.0), axis=1, keepdims=True)

    def expert_in(u, gcol):
        return jnp.where(gcol > 0.0, u, 0.0).astype(BF)

    x1[own_rows, :] = tok[...]
    slot = lax.broadcasted_iota(jnp.int32, (LANES, T), 0)
    table = jnp.zeros((LANES, T), F32)
    for l in range(2):
        for j in range(6):
            table = table + jnp.where(slot == ids[j, l:l + 1, :] + 64 * l, gates[j, l:l + 1, :], 0.0)
    gt[own_rows, :] = table.T
    dyg[z, home_unit, :] = dout[...]
    pl.semaphore_wait(barrier, len(peers))

    def row_view(buf):
        return lambda dz, dy: buf.at[pl.ds(rows_at[T][dz][dy], T), :]

    ag_tok = Gather(row_view(x1), 0, 0)
    ag_gt = Gather(row_view(gt), 1, 1)
    ag_dy = ColumnGather()
    ag_x2 = Gather(row_view(x2), 0, 2)
    ag_du2 = Gather(row_view(du2), 1, 3)
    ag_tok.start()
    ag_gt.start()
    ag_dy.start()

    for load in loads:
        load.wait()
    for l in range(2):
        for e in range(2):
            for p in range(3):
                w3[l, e, FP * p + FF:FP * p + FP, :] = jnp.zeros((FP - FF, D), BF)

    def gate_up(l, e):
        return w3[l, e, 0:2 * FP, :]

    def down(l, e):
        return w3[l, e, 2 * FP:, :]

    @pl.loop(0, 8)
    def _(k):
        for kk in range(8):
            @pl.when(k == kk)
            def _(kk=kk):
                ag_tok.chunk(kk)
                ag_gt.chunk(kk)
                if kk % 2:
                    ag_dy.zpoll(kk // 2 + 1)
        rows = plane_rows(k)
        xc = x1[rows, :]
        u = (xc.astype(F32) + dot(xc, wmix[0])).astype(BF)
        u1[rows, :] = u
        uf = u.astype(F32)
        total = jnp.zeros((CH, D), F32)
        for e in range(2):
            gcol = gate_col(0, e, rows)
            pre = dot_nt(expert_in(uf, gcol), gate_up(0, e))
            ab[e, rows, :] = pre
            a, b = pre[:, :FP], pre[:, FP:]
            h = (a * jax.nn.sigmoid(a) * b).astype(BF)
            hb[0, e, rows, :] = h
            total = total + gcol * dot(h, down(0, e)).astype(BF).astype(F32)
        pacc[rows, :] = total

    rs = Scatter(pacc, 0)
    for s in range(5):
        rs.round(s)
        if s == 1:
            ag_dy.ypoll(1)
    rs.y_start()
    ag_tok.drain()
    ag_gt.drain()
    y1 = (u1[own_rows, :].astype(F32) + rs.finish()).astype(BF)
    x2[own_rows, :] = y1
    ag_x2.start()
    rs.drain()
    ag_dy.ypoll(2)
    ag_dy.drain()

    def backward_part(layer, e, rows, gcol, dyc, pre):
        a, b = pre[:, :FP], pre[:, FP:]
        c = (gcol * dyc).astype(BF)
        cb_[e, rows, :] = c
        dh = dot_nt(c, down(layer, e))
        s = jax.nn.sigmoid(a)
        dab[e, rows, 0:FP] = (dh * b * (s * (1.0 + a * (1.0 - s)))).astype(BF)
        dab[e, rows, FP:] = (dh * (a * s)).astype(BF)
        v = dot(dab[e, rows, :], gate_up(layer, e)).astype(BF)
        return gcol * v.astype(F32)

    @pl.loop(0, 8)
    def _(k):
        for kk in range(8):
            @pl.when(k == kk)
            def _(kk=kk):
                ag_x2.chunk(kk)
        rows = plane_rows(k)
        xc = x2[rows, :]
        u = (xc.astype(F32) + dot(xc, wmix[1])).astype(BF)
        u2[rows, :] = u
        uf = u.astype(F32)
        dyc = dyg[plane_of(k)].astype(F32)
        total = jnp.zeros((CH, D), F32)
        back = jnp.zeros((CH, D), F32)
        for e in range(2):
            gcol = gate_col(1, e, rows)
            pre = dot_nt(expert_in(uf, gcol), gate_up(1, e))
            a, b = pre[:, :FP], pre[:, FP:]
            h = (a * jax.nn.sigmoid(a) * b).astype(BF)
            hb[1, e, rows, :] = h
            total = total + gcol * dot(h, down(1, e)).astype(BF).astype(F32)
            back = back + backward_part(1, e, rows, gcol, dyc, pre)
        pacc2[rows, :] = total
        pacc[rows, :] = back

    def weight_grads(layer, e, ug):
        @pl.loop(0, 6)
        def _(i):
            part = lax.div(i, 3)
            cols = pl.ds(pl.multiple_of(i * LANES, LANES), LANES)
            rows = pl.ds(pl.multiple_of(part * FF + (i - 3 * part) * LANES, 32), LANES)
            grad[layer, e, rows, :] = dot_tn(dab[e, :, cols], ug[...]).astype(BF)

        @pl.loop(0, 3)
        def _(i):
            cols = pl.ds(pl.multiple_of(i * LANES, LANES), LANES)
            rows = pl.ds(pl.multiple_of(2 * FF + i * LANES, 32), LANES)
            grad[layer, e, rows, :] = dot_tn(hb[layer, e, :, cols], cb_[e]).astype(BF)

    rs = Scatter(pacc, 1)
    rs.round(0)
    weight_grads(1, 1 - core, u2)
    ar2 = Reduce(1)
    ar2.stage(0)
    rs.round(1)
    weight_grads(1, core, u2)
    rs.round(2)
    ar2.stage(1)
    for s in range(3, 5):
        rs.round(s)
    rs.y_start()
    ag_x2.drain()
    du2[own_rows, :] = (dout[...].astype(F32) + rs.finish()).astype(BF)
    ag_du2.start()
    rs.drain()

    @pl.loop(0, 8)
    def _(k):
        for kk in range(8):
            @pl.when(k == kk)
            def _(kk=kk):
                ag_du2.chunk(kk)
                if kk == 1:
                    ar2.stage(2)
                if kk == 4:
                    ar2.stage(3)
                if kk == 7:
                    ar2.stage(4)
        rows = plane_rows(k)
        duc = du2[rows, :]
        dyc = (duc.astype(F32) + dot_nt(duc, wmix[1])).astype(BF)
        dyg[plane_of(k)] = dyc
        dyc = dyc.astype(F32)
        back = jnp.zeros((CH, D), F32)
        for e in range(2):
            back = back + backward_part(0, e, rows, gate_col(0, e, rows), dyc, ab[e, rows, :])
        pacc[rows, :] = back

    rs = Scatter(pacc, 2)
    rs_y2 = Scatter(pacc2, 3)
    rs.round(0)
    weight_grads(0, 1 - core, u1)
    ar1 = Reduce(0)
    ar1.stage(0)
    mix_scatter_start()
    rs.round(1)
    mix_start(1, x2, du2)
    weight_grads(0, core, u1)
    ar1.stage(1)
    rs.round(2)
    mix_sum(1)
    ar2.stage(5)
    rs.round(3)
    mix_scatter_turn()
    rs.round(4)
    rs.y_start()
    ar1.stage(2)
    rs_y2.round(0)
    ar2.stage(6)
    d_u1 = (dyg[z, home_unit, :].astype(F32) + rs.finish()).astype(BF)
    dx_out[...] = (d_u1.astype(F32) + dot_nt(d_u1, wmix[0])).astype(BF)
    mix_scatter_sum()
    rs_y2.round(1)
    mix_gather_start(1)
    ar1.stage(3)
    rs_y2.round(2)
    mix_sum(0)
    mix_gather_start(0)
    rs_y2.round(3)
    ar1.stage(4)
    rs_y2.round(4)
    rs_y2.y_start()
    ar2.stage(7)
    ag_du2.drain()
    rs.drain()
    mix_scatter_drain()
    mix_gather_done(1)
    ar1.stage(5)
    y_out[...] = (u2[own_rows, :].astype(F32) + rs_y2.finish()).astype(BF)
    mix_swap_done(1)
    dmix_out[1] = dm_all[1]
    mix_gather_done(0)
    ar1.stage(6)
    mix_swap_done(0)
    dmix_out[0] = dm_all[0]
    rs_y2.drain()
    ar1.stage(7)


def copy_kernel(*refs):
    n = len(refs) // 3
    src, dst, buf, sem = refs[:n], refs[n:2 * n], refs[2 * n:3 * n], refs[3 * n]
    loads = [pltpu.make_async_copy(src[i], buf[i], sem.at[0, i]) for i in range(n)]
    stores = [pltpu.make_async_copy(buf[i], dst[i], sem.at[1, i]) for i in range(n)]
    for load in loads:
        load.start()
    for load, store in zip(loads, stores):
        load.wait()
        store.start()
    for store in stores:
        store.wait()


def solution(mesh):
    tok_spec = P(('dp', 'ep'))
    route_spec = P(None, ('dp', 'ep'))
    whole_spec = P()
    expert_spec = P(None, 'ep')

    def device_step(tokens, d_out, expert_ids, gate_vals, w_mix, w_gate, w_up, w_down):
        vm = pl.BlockSpec(memory_space=pltpu.VMEM)
        hbm = pl.BlockSpec(memory_space=pl.ANY)
        shape = jax.ShapeDtypeStruct
        dma = pltpu.SemaphoreType.DMA
        wg_t, wu_t = jnp.swapaxes(w_gate, 2, 3), jnp.swapaxes(w_up, 2, 3)
        results = pl.pallas_call(
            step_kernel,
            out_shape=(shape((T, D), BF), shape((T, D), BF), shape((2, D, D), BF),
                       *[shape(both(FF, D), BF)] * 3),
            in_specs=[vm] * 5 + [hbm] * 3,
            out_specs=(vm,) * 3 + (hbm,) * 3,
            scratch_shapes=[
                vmem(both(3 * FP, D)),
                *[vmem((NT, D))] * 2, vmem((NZ, CH, D)), *[vmem((NT, D))] * 4,
                vmem((NT, LANES), F32), vmem((2, NT, 2 * FP), F32),
                vmem(both(NT, FP)), vmem((2, NT, 2 * FP)), vmem((2, NT, D)),
                vmem((NT, D), F32), vmem((NT, D), F32),
                vmem((4, 2, CH, D)), vmem((4, 2, 3, CH, D)), vmem((4, 2, CH, D)),
                vmem((4, 3, T, D)), vmem((4, 3, T, D)),
                vmem(both(GR + 32, D)), vmem((2, GR, D)), vmem((2, 6, HR, LANES)), vmem(both(GR, D)),
                vmem((LANES, D), F32), vmem((2, SL, D), F32), vmem((2, SL, D)), vmem((2, 7, SL, D)),
                vmem((2, D, D)), vmem((NZ, NY * SL, D)), vmem((NZ, SL, D)),
                vmem((NY, NZ, SL, D)), vmem((NZ, SL, D)),
                dma((3, 2, 2)),
                dma((2, 3)), dma((4, 3)), dma((2, *ZSEM)), dma((4, *ZSEM)),
                dma((2, *ZSEM)), dma((4, *ZSEM)), dma((2, 3)), dma((4, 3)),
                *[dma((2, 12))] * 2, *[dma((2, 7))] * 2, dma((2, 2, 3)), *[dma((2, 6))] * 2,
                *[dma((2, NEP))] * 2, *[dma((NEP,))] * 2,
            ],
            compiler_params=pltpu.CompilerParams(
                collective_id=0, has_side_effects=True, vmem_limit_bytes=67043328),
        )(tokens, d_out, jnp.transpose(expert_ids, (2, 0, 1)), jnp.transpose(gate_vals, (2, 0, 1)),
          w_mix, wg_t, wu_t, w_down)
        y, dx, dmix, dg_t, du_t, dw = pl.pallas_call(
            copy_kernel,
            out_shape=[shape(r.shape, r.dtype) for r in results],
            in_specs=[hbm] * 6,
            out_specs=[hbm] * 6,
            scratch_shapes=[vmem(r.shape) for r in results] + [dma((2, 6))],
        )(*results)
        return y, dx, dmix, jnp.swapaxes(dg_t, 2, 3), jnp.swapaxes(du_t, 2, 3), dw

    return jax.shard_map(device_step, mesh=mesh,
                         in_specs=(tok_spec, tok_spec, route_spec, route_spec, whole_spec,
                                   expert_spec, expert_spec, expert_spec),
                         out_specs=(tok_spec, tok_spec, whole_spec, expert_spec, expert_spec, expert_spec),
                         check_vma=False)
```
